256 devices in a mesh: gx: 16 (over y_hi, z), gy: 4 (over x), gz: 4 (over y_lo, core).
Axes of the slice: x: 4, y: 4 (y_hi: 2, y_lo: 2; y = y_hi * 2 + y_lo), z: 8, core: 2. Of those that a mesh axis runs over, the one named last changes fastest.
Arguments:
- fields: float32 [4, 64, 256, 512], P(None, 'gx', 'gy', 'gz'), may hold values from -8 to 8
- volume_code: int32 [64, 256, 512], P('gx', 'gy', 'gz'), may hold values from 65536 to 1048576
- cut_flag: int32 [64, 256, 512], P('gx', 'gy', 'gz'), may hold values 0 or 1
- member_bits: int32 [64, 256, 512], P('gx', 'gy', 'gz'), may hold values from 0 to 134217727
Outputs:
- merged: float32 [4, 64, 256, 512], P(None, 'gx', 'gy', 'gz')
The draws below stay inside these ranges and needn't reach their ends.
All inputs are finite; a program needn't handle non-finite values. No bound on the sum of `cut_flag` on one device may be relied on, other than what follows from the above.
Results may differ from the reference program's by a relative error of at most 0.00015.
Values sent between devices are 32-bit elements; how exact they have to be, the bound alone decides.
A program may use at most 128 MiB of HBM per device.

```python
import jax
import jax.numpy as jnp

FIELDS = 4
PASSES = 2
NX = 64
NY = 256
NZ = 512


def set_ends(result, stream_key, low, largest):
    extent = result.shape
    index_at = [jax.random.randint(jax.random.fold_in(stream_key, axis), (), 0, extent[axis]) for axis in range(len(extent))]
    result = result.at[tuple(index_at)].set(low)
    longest = extent.index(max(extent))
    index_at[longest] = (index_at[longest] + 1) % extent[longest]
    return result.at[tuple(index_at)].set(largest)


def steps_of(stream_key, shape, cuts, low, largest):
    factor_of, own = 1.0, jax.random.fold_in(stream_key, 6)
    for dim, shards_of in cuts:
        draws = jnp.exp(jax.random.uniform(jax.random.fold_in(own, dim), (shards_of,), jnp.float32, low / len(cuts), largest / len(cuts)))
        factor_of = factor_of * jnp.repeat(draws, shape[dim] // shards_of).reshape([-1 if axis == dim else 1 for axis in range(len(shape))])
    return factor_of


def normal_values(key, shape, spread, bound, pieces=(), kind=jnp.bfloat16):
    values = jax.random.normal(key, shape, jnp.float32) * spread
    if len(pieces) > 0:
        values = steps_of(key, shape, pieces, -0.22, 0.18) * values
    return jnp.clip(values, min=-bound, max=bound).astype(kind)


def setup_inputs(seed: int = 0) -> dict:
    streams_of = jax.random.split(jax.random.key(seed), 5)
    return {
        "fields": normal_values(streams_of[0], (FIELDS, NX, NY, NZ), 1.0, 8.0, ((1, 16), (2, 4), (3, 4)), jnp.float32),
        "volume_code": set_ends(jax.random.randint(streams_of[1], (NX, NY, NZ), 65536, 1048577), jax.random.fold_in(streams_of[1], 1), 65536, 1048576).astype(jnp.int32),
        "cut_flag": set_ends((jax.random.randint(streams_of[2], (NX, NY, NZ), 0, 3) < 1).astype(jnp.int32), jax.random.fold_in(streams_of[2], 1), 0, 1),
        "member_bits": set_ends(jax.random.randint(streams_of[3], (NX, NY, NZ), 0, 134217728), jax.random.fold_in(streams_of[3], 1), 0, 134217727).astype(jnp.int32),
    }


def reference(fields, volume_code, cut_flag, member_bits):
    kappa = volume_code.astype(jnp.float32) / 1048576.0
    active = member_bits * cut_flag
    offsets = []
    for dx in (-1, 0, 1):
        for dy in (-1, 0, 1):
            for dz in (-1, 0, 1):
                offsets.append((dx, dy, dz))
    state = fields
    for step in range(PASSES):
        volume = jnp.zeros_like(kappa)
        mass = jnp.zeros_like(fields)
        count = jnp.zeros_like(kappa)
        weighted = kappa[None] * state
        for index, shift in enumerate(offsets):
            if index == 13:
                member = jnp.ones_like(kappa)
            else:
                member = jnp.bitwise_and(jnp.right_shift(active, index), 1).astype(jnp.float32)
            volume = volume + jnp.roll(member * kappa, shift, axis=(0, 1, 2))
            mass = mass + jnp.roll(member[None] * weighted, shift, axis=(1, 2, 3))
        hat = mass / volume[None]
        total = jnp.zeros_like(fields)
        for index, shift in enumerate(offsets):
            if index == 13:
                member = jnp.ones_like(kappa)
            else:
                member = jnp.bitwise_and(jnp.right_shift(active, index), 1).astype(jnp.float32)
            back = (-shift[0], -shift[1], -shift[2])
            total = total + member[None] * jnp.roll(hat, back, axis=(1, 2, 3))
            count = count + member
        state = total / count[None]
    return state
```

```python
import jax
import jax.numpy as jnp
from jax import lax
from jax.experimental import pallas as pl
from jax.experimental.pallas import tpu as pltpu
from jax.sharding import PartitionSpec as P

MESH = pl.DeviceIdType.MESH
FIELDS = 4
LAYERS = 4
ROWS = 64
TILES = ROWS // 8
PADDED = ROWS + 16
LANES = 128
SIGNS = (-1, 1)

TRAVEL = []
for kind in ((1, 0, 0), (1, 1, 0), (1, 0, 1), (1, 1, 1), (0, 0, 1), (0, 1, 0), (0, 1, 1)):
    for sx in SIGNS if kind[0] else (0,):
        for sy in SIGNS if kind[1] else (0,):
            for sz in SIGNS if kind[2] else (0,):
                TRAVEL.append((sx, sy, sz))


def side(sign):
    return (sign + 1) // 2


def offset_bit(dx, dy, dz):
    return 9 * (dx + 1) + 3 * (dy + 1) + (dz + 1)


def neighbour(travel):
    result = {}
    for axis, sign in zip(("gx", "gy", "gz"), travel):
        if sign:
            count = lax.axis_size(axis)
            result[axis] = lax.rem(lax.axis_index(axis) + sign + count, count)
    return result


def turn(value, shift):
    if isinstance(shift, int):
        shift = shift % LANES
        if shift == 0:
            return value
    return pltpu.roll(value, shift, 1)


def kernel(fields, volume_code, cut_flag, member_bits, out, raw, code, cut, bits, act, kap, inv_count,
           inv_volume, w, acc, result, hats, xface, yrows, edges, zpack, xzpack, yzpack, cpack,
           rx, ry, re, rz, rxz, ryz, rc, in_sem, out_sem, send_sem, recv_sem):
    lane8 = lax.broadcasted_iota(jnp.int32, (8, LANES), 1)
    lane1 = lax.broadcasted_iota(jnp.int32, (1, LANES), 1)
    zero8 = jnp.zeros((8, LANES), jnp.float32)

    loads = []
    for index, (source, target) in enumerate(
        ((volume_code, code), (cut_flag, cut), (member_bits, bits), (fields, raw))
    ):
        copy = pltpu.make_async_copy(source, target, in_sem.at[index])
        copy.start()
        loads.append(copy)
    barrier = pltpu.get_barrier_semaphore()
    for travel in TRAVEL:
        pl.semaphore_signal(barrier, inc=1, device_id=neighbour(travel), device_id_type=MESH)

    for x in range(LAYERS):
        for rows in (0, PADDED - 8):
            act[x, rows : rows + 8, :] = jnp.zeros((8, LANES), jnp.int32)
            for f in range(FIELDS + 1):
                w[f, x, rows : rows + 8, :] = zero8
    for copy in loads:
        copy.wait()

    def prepare(t, carry):
        own = pl.ds(pl.multiple_of(8 * t, 8), 8)
        padded = pl.ds(pl.multiple_of(8 * t + 8, 8), 8)
        for x in range(LAYERS):
            kappa = code[x, own, :].astype(jnp.float32) * (1.0 / 1048576.0)
            active = bits[x, own, :] * cut[x, own, :]
            act[x, padded, :] = active
            kap[x, own, :] = kappa
            others = lax.population_count(jnp.bitwise_and(active, ((1 << 27) - 1) ^ (1 << 13)))
            inv_count[x, own, :] = 1.0 / (others + 1).astype(jnp.float32)
            w[FIELDS, x, padded, :] = kappa
            for f in range(FIELDS):
                w[f, x, padded, :] = kappa * raw[f, x, own, :]
        return carry

    lax.fori_loop(0, TILES, prepare, 0)
    pl.semaphore_wait(barrier, len(TRAVEL))

    def message(stage, travel):
        sx, sy, sz = travel
        count = FIELDS + 1 if stage == 0 else FIELDS
        ix, iy, iz = side(sx), side(sy), side(sz)
        e = 2 * ix + iy
        if sx and not sy and not sz:
            if stage % 2 == 0:
                source, target = xface.at[stage // 2, ix, 0:count], rx.at[stage // 2, ix, 0:count]
            else:
                mid = hats.at[stage // 2, 1]
                source = mid.at[:, 4 if sx == 1 else 1, 8 : 8 + ROWS, :]
                target = mid.at[:, 0 if sx == 1 else 5, 8 : 8 + ROWS, :]
        elif sy and not sx and not sz:
            source, target = yrows.at[stage, iy], ry.at[stage, iy]
        elif sz and not sx and not sy:
            source, target = zpack.at[stage], rz.at[stage, iz]
        elif sx and sy and not sz:
            source, target = edges.at[stage, e], re.at[stage, e]
        elif sx and sz and not sy:
            source, target = xzpack.at[stage, ix], rxz.at[stage, ix, iz]
        elif sy and sz and not sx:
            source, target = yzpack.at[stage, iy], ryz.at[stage, iy, iz]
        else:
            source, target = cpack.at[stage, e], rc.at[stage, e, iz]
        index = TRAVEL.index(travel)
        return pltpu.make_async_remote_copy(
            src_ref=source,
            dst_ref=target,
            send_sem=send_sem.at[stage, index],
            recv_sem=recv_sem.at[stage, index],
            device_id=neighbour(travel),
            device_id_type=MESH,
        )

    started = []

    def send(stage, chosen):
        for travel in TRAVEL:
            if chosen(*travel):
                copy = message(stage, travel)
                copy.start()
                started.append(copy)

    def receive(stage, chosen):
        for travel in TRAVEL:
            if chosen(*travel):
                message(stage, travel).wait_recv()

    def pushed(xt, row, dys, count):
        sums = [[None] * count for _ in range(3)]
        for dx in (-1, 0, 1):
            xs = xt - dx
            if xs < 0 or xs >= LAYERS:
                continue
            for dy in dys:
                rows = pl.ds(row - dy, 8)
                active = act[xs, rows, :]
                values = [w[f, xs, rows, :] for f in range(count)]
                for dz in (-1, 0, 1):
                    bit = offset_bit(dx, dy, dz)
                    if bit != 13:
                        chosen = jnp.bitwise_and(active, 1 << bit) != 0
                    for f in range(count):
                        term = values[f] if bit == 13 else jnp.where(chosen, values[f], 0.0)
                        old = sums[dz + 1][f]
                        sums[dz + 1][f] = term if old is None else old + term
        mains, ends = [], []
        for f in range(count):
            up = turn(sums[2][f], 1)
            down = turn(sums[0][f], -1)
            mains.append(
                sums[1][f] + jnp.where(lane8 == 0, 0.0, up) + jnp.where(lane8 == LANES - 1, 0.0, down)
            )
            ends.append(jnp.where(lane8 < LANES // 2, up, down))
        return mains, ends

    def packed(base, value, p, lane):
        return jnp.where(jnp.right_shift(lane, 1) == p, turn(value, 1 + 2 * p), base)

    def scatter(stage, count):
        for sx in SIGNS:
            xt = -1 if sx == -1 else LAYERS
            ix = side(sx)

            def layer(t, pack, xt=xt, ix=ix):
                mains, ends = pushed(xt, 8 * t + 8, (-1, 0, 1), count)
                own = pl.ds(pl.multiple_of(8 * t, 8), 8)
                small = zero8
                for f in range(count):
                    xface[stage // 2, ix, f, own, :] = mains[f]
                    small = packed(small, ends[f], f, lane8)
                start = 2 * count * t
                inside = (lane8 >= start) & (lane8 < start + 2 * count)
                return jnp.where(inside, turn(small, start), pack)

            xzpack[stage, ix] = lax.fori_loop(0, TILES, layer, zero8)
            send(stage, lambda a, b, c: (a, b, c) == (sx, 0, 0))
        for sx in SIGNS:
            xt = -1 if sx == -1 else LAYERS
            for sy in SIGNS:
                mains, ends = pushed(xt, 0 if sy == -1 else PADDED - 8, (sy,), count)
                row = 7 if sy == -1 else 0
                e = 2 * side(sx) + side(sy)
                small = zero8
                for f in range(count):
                    edges[stage, e, f : f + 1, :] = mains[f][row : row + 1, :]
                    small = packed(small, ends[f], f, lane8)
                cpack[stage, e] = small[row : row + 1, :]
        send(stage, lambda a, b, c: a != 0 and (b != 0 or c != 0))

        def rest(t, carry):
            own = pl.ds(pl.multiple_of(8 * t, 8), 8)
            pack = zero8
            for xt in range(LAYERS):
                mains, ends = pushed(xt, 8 * t + 8, (-1, 0, 1), count)
                for f in range(count):
                    acc[f, xt, own, :] = mains[f]
                    pack = packed(pack, ends[f], 4 * f + xt, lane8)
            zpack[stage, t] = pack
            return carry

        lax.fori_loop(0, TILES, rest, 0)
        send(stage, lambda a, b, c: (a, b) == (0, 0))
        for sy in SIGNS:
            row = 7 if sy == -1 else 0
            pack = zero8
            for xt in range(LAYERS):
                mains, ends = pushed(xt, 0 if sy == -1 else PADDED - 8, (sy,), count)
                for f in range(count):
                    p = 4 * f + xt
                    yrows[stage, side(sy), p : p + 1, :] = mains[f][row : row + 1, :]
                    pack = packed(pack, ends[f], p, lane8)
            yzpack[stage, side(sy)] = pack[row : row + 1, :]
        send(stage, lambda a, b, c: a == 0 and b != 0)

    def edge_lanes(value, lane):
        return jnp.where((lane == 0) | (lane == LANES - 1), value, 0.0)

    def merged_pairs(up, down, lane):
        return jnp.where(jnp.bitwise_and(lane, 1) == 1, up, down)

    def combine(stage, count):
        odd = stage + 1
        which = stage // 2
        receive(stage, lambda a, b, c: True)
        for sy in SIGNS:
            iy = side(sy)
            row = 0 if sy == 1 else ROWS - 1
            yz = merged_pairs(ryz[stage, iy, 1], ryz[stage, iy, 0], lane1)
            for x in range(LAYERS):
                sx = 1 if x == 0 else -1 if x == LAYERS - 1 else 0
                if sx:
                    e = 2 * side(sx) + iy
                    corner = merged_pairs(rc[stage, e, 1], rc[stage, e, 0], lane1)
                for f in range(count):
                    p = 4 * f + x
                    value = ry[stage, iy, p : p + 1, :]
                    ends = turn(yz, LANES - 1 - 2 * p)
                    if sx:
                        value = value + re[stage, e, f : f + 1, :]
                        ends = ends + turn(corner, LANES - 1 - 2 * f)
                    acc[f, x, row : row + 1, :] += value + edge_lanes(ends, lane1)

        def group(layers, first):
            def tile(t, packs):
                own = pl.ds(pl.multiple_of(8 * t, 8), 8)
                padded = pl.ds(pl.multiple_of(8 * t + 8, 8), 8)
                z = merged_pairs(rz[stage, 1, t], rz[stage, 0, t], lane8)
                pack = zero8 if first else zpack[odd, t]
                packs = list(packs)
                for x in layers:
                    sx = 1 if x == 0 else -1 if x == LAYERS - 1 else 0
                    if sx:
                        xz = merged_pairs(rxz[stage, side(sx), 1], rxz[stage, side(sx), 0], lane8)
                        xz = turn(xz, LANES - 1 - 2 * count * t)
                    sums = []
                    for f in range(count):
                        value = acc[f, x, own, :]
                        ends = turn(z, LANES - 1 - 2 * (4 * f + x))
                        if sx:
                            value = value + rx[which, side(sx), f, own, :]
                            ends = ends + turn(xz, -2 * f)
                        sums.append(value + edge_lanes(ends, lane8))
                    if stage == 0:
                        inverse = 1.0 / sums[FIELDS]
                        inv_volume[x, own, :] = inverse
                    else:
                        inverse = inv_volume[x, own, :]
                    small = zero8
                    for f in range(FIELDS):
                        hat = sums[f] * inverse
                        hats[which, 1, f, x + 1, padded, :] = hat
                        pack = packed(pack, hat, 4 * f + x, lane8)
                        if sx:
                            small = packed(small, hat, f, lane8)
                    if sx:
                        start = 2 * FIELDS * t
                        inside = (lane8 >= start) & (lane8 < start + 2 * FIELDS)
                        slot = side(-sx)
                        packs[slot] = jnp.where(inside, turn(small, start), packs[slot])
                zpack[odd, t] = pack
                return tuple(packs)

            return lax.fori_loop(0, TILES, tile, (zero8, zero8))

        packs = group((0, LAYERS - 1), True)
        send(odd, lambda a, b, c: a != 0 and b == 0 and c == 0)
        for sx in SIGNS:
            xzpack[odd, side(sx)] = packs[side(sx)]
            x = 0 if sx == -1 else LAYERS - 1
            for sy in SIGNS:
                row = 8 if sy == -1 else 7 + ROWS
                e = 2 * side(sx) + side(sy)
                small = jnp.zeros((1, LANES), jnp.float32)
                for f in range(FIELDS):
                    value = hats[which, 1, f, x + 1, row : row + 1, :]
                    edges[odd, e, f : f + 1, :] = value
                    small = packed(small, value, f, lane1)
                cpack[odd, e] = small
        send(odd, lambda a, b, c: a != 0 and (b != 0 or c != 0))
        group(tuple(range(1, LAYERS - 1)), False)
        send(odd, lambda a, b, c: (a, b) == (0, 0))
        for sy in SIGNS:
            row = 8 if sy == -1 else 7 + ROWS
            for x in range(LAYERS):
                for f in range(FIELDS):
                    p = 4 * f + x
                    yrows[odd, side(sy), p : p + 1, :] = hats[which, 1, f, x + 1, row : row + 1, :]
            t = 0 if sy == -1 else TILES - 1
            yzpack[odd, side(sy)] = zpack[odd, t, row % 8 : row % 8 + 1, :]
        send(odd, lambda a, b, c: a == 0 and b != 0)

    def swapped_pairs(from_below, from_above, lane):
        return jnp.where(jnp.bitwise_and(lane, 1) == 1, turn(from_below, 1), turn(from_above, -1))

    def store_shifted(which, f, xi, rows, value, ends, lane):
        hats[which, 2, f, xi, rows, :] = jnp.where(lane == LANES - 1, ends, turn(value, -1))
        hats[which, 0, f, xi, rows, :] = jnp.where(lane == 0, ends, turn(value, 1))

    def gather(stage, last):
        which = stage // 2
        receive(stage, lambda a, b, c: True)
        for sy in SIGNS:
            iy = side(sy)
            row = 7 if sy == 1 else 8 + ROWS
            rows = slice(row, row + 1)
            yz = swapped_pairs(ryz[stage, iy, 1], ryz[stage, iy, 0], lane1)
            for x in range(-1, LAYERS + 1):
                sx = 1 if x == -1 else -1 if x == LAYERS else 0
                if sx:
                    e = 2 * side(sx) + iy
                    corner = swapped_pairs(rc[stage, e, 1], rc[stage, e, 0], lane1)
                for f in range(FIELDS):
                    p = 4 * f + x
                    if sx:
                        value = re[stage, e, f : f + 1, :]
                        ends = turn(corner, LANES - 1 - 2 * f)
                    else:
                        value = ry[stage, iy, p : p + 1, :]
                        ends = turn(yz, LANES - 1 - 2 * p)
                    hats[which, 1, f, x + 1, rows, :] = value
                    store_shifted(which, f, x + 1, rows, value, ends, lane1)

        def shifts(t, carry):
            padded = pl.ds(pl.multiple_of(8 * t + 8, 8), 8)
            z = swapped_pairs(rz[stage, 1, t], rz[stage, 0, t], lane8)
            for x in range(-1, LAYERS + 1):
                sx = 1 if x == -1 else -1 if x == LAYERS else 0
                if sx:
                    xz = swapped_pairs(rxz[stage, side(sx), 1], rxz[stage, side(sx), 0], lane8)
                    xz = turn(xz, LANES - 1 - 2 * FIELDS * t)
                for f in range(FIELDS):
                    ends = turn(xz, -2 * f) if sx else turn(z, LANES - 1 - 2 * (4 * f + x))
                    value = hats[which, 1, f, x + 1, padded, :]
                    store_shifted(which, f, x + 1, padded, value, ends, lane8)
            return carry

        lax.fori_loop(0, TILES, shifts, 0)

        def tile(t, carry):
            own = pl.ds(pl.multiple_of(8 * t, 8), 8)
            padded = pl.ds(pl.multiple_of(8 * t + 8, 8), 8)
            for x in range(LAYERS):
                active = act[x, padded, :]
                sums = [hats[which, 1, f, x + 1, padded, :] for f in range(FIELDS)]
                for dx in (-1, 0, 1):
                    for dy in (-1, 0, 1):
                        for dz in (-1, 0, 1):
                            bit = offset_bit(dx, dy, dz)
                            if bit == 13:
                                continue
                            chosen = jnp.bitwise_and(active, 1 << bit) != 0
                            rows = pl.ds(8 * t + 8 + dy, 8)
                            for f in range(FIELDS):
                                value = hats[which, dz + 1, f, x + 1 + dx, rows, :]
                                sums[f] = sums[f] + jnp.where(chosen, value, 0.0)
                scale = inv_count[x, own, :]
                if not last:
                    scale = scale * kap[x, own, :]
                for f in range(FIELDS):
                    if last:
                        result[f, x, own, :] = sums[f] * scale
                    else:
                        w[f, x, padded, :] = sums[f] * scale
            return carry

        lax.fori_loop(0, TILES, tile, 0)

    scatter(0, FIELDS + 1)
    combine(0, FIELDS + 1)
    gather(1, False)
    scatter(2, FIELDS)
    combine(2, FIELDS)
    gather(3, True)
    copy = pltpu.make_async_copy(result, out, out_sem)
    copy.start()
    for sent in started:
        sent.wait_send()
    copy.wait()


def body(fields, volume_code, cut_flag, member_bits):
    f32, i32 = jnp.float32, jnp.int32
    vmem = pltpu.VMEM
    block = (LAYERS, ROWS, LANES)
    padded = (LAYERS, PADDED, LANES)
    row_count = 24
    scratch = [
        vmem((FIELDS,) + block, f32),
        vmem(block, i32),
        vmem(block, i32),
        vmem(block, i32),
        vmem(padded, i32),
        vmem(block, f32),
        vmem(block, f32),
        vmem(block, f32),
        vmem((FIELDS + 1,) + padded, f32),
        vmem((FIELDS + 1,) + block, f32),
        vmem((FIELDS,) + block, f32),
        vmem((2, 3, FIELDS, LAYERS + 2, PADDED, LANES), f32),
        vmem((2, 2, FIELDS + 1, ROWS, LANES), f32),
        vmem((4, 2, row_count, LANES), f32),
        vmem((4, 4, 8, LANES), f32),
        vmem((4, TILES, 8, LANES), f32),
        vmem((4, 2, 8, LANES), f32),
        vmem((4, 2, 1, LANES), f32),
        vmem((4, 4, 1, LANES), f32),
        vmem((2, 2, FIELDS + 1, ROWS, LANES), f32),
        vmem((4, 2, row_count, LANES), f32),
        vmem((4, 4, 8, LANES), f32),
        vmem((4, 2, TILES, 8, LANES), f32),
        vmem((4, 2, 2, 8, LANES), f32),
        vmem((4, 2, 2, 1, LANES), f32),
        vmem((4, 4, 2, 1, LANES), f32),
        pltpu.SemaphoreType.DMA((4,)),
        pltpu.SemaphoreType.DMA,
        pltpu.SemaphoreType.DMA((4, len(TRAVEL))),
        pltpu.SemaphoreType.DMA((4, len(TRAVEL))),
    ]
    anywhere = pl.BlockSpec(memory_space=pl.ANY)
    return pl.pallas_call(
        kernel,
        out_shape=jax.ShapeDtypeStruct((FIELDS,) + block, f32),
        in_specs=[anywhere] * 4,
        out_specs=anywhere,
        scratch_shapes=scratch,
        compiler_params=pltpu.CompilerParams(
            collective_id=0, has_side_effects=True, vmem_limit_bytes=48 * 1024 * 1024
        ),
    )(fields, volume_code, cut_flag, member_bits)


def solution(mesh):
    in_specs = (
        P(None, "gx", "gy", "gz"),
        P("gx", "gy", "gz"),
        P("gx", "gy", "gz"),
        P("gx", "gy", "gz"),
    )
    out_specs = P(None, "gx", "gy", "gz")
    return jax.shard_map(body, mesh=mesh, in_specs=in_specs, out_specs=out_specs, check_vma=False)
```

```python
import jax
import jax.numpy as jnp
from jax import lax
from jax.experimental import pallas as pl
from jax.experimental.pallas import tpu as pltpu
from jax.sharding import PartitionSpec as P

MESH = pl.DeviceIdType.MESH
FIELDS = 4
LAYERS = 4
ROWS = 64
TILES = ROWS // 8
PADDED = ROWS + 16
LANES = 128
CHUNK = 16
CHUNKS = ROWS // CHUNK
SIGNS = (-1, 1)

TRAVEL = []
for kind in ((1, 0, 0), (1, 1, 0), (1, 0, 1), (1, 1, 1), (0, 0, 1), (0, 1, 0), (0, 1, 1)):
    for sx in SIGNS if kind[0] else (0,):
        for sy in SIGNS if kind[1] else (0,):
            for sz in SIGNS if kind[2] else (0,):
                TRAVEL.append((sx, sy, sz))
MESSAGES = []
for travel in TRAVEL:
    for chunk in range(CHUNKS if travel[1:] == (0, 0) else 1):
        MESSAGES.append(travel + (chunk,))


def side(sign):
    return (sign + 1) // 2


def offset_bit(dx, dy, dz):
    return 9 * (dx + 1) + 3 * (dy + 1) + (dz + 1)


def neighbour(travel):
    result = {}
    for axis, sign in zip(("gx", "gy", "gz"), travel):
        if sign:
            count = lax.axis_size(axis)
            result[axis] = lax.rem(lax.axis_index(axis) + sign + count, count)
    return result


def turn(value, shift):
    if isinstance(shift, int):
        shift = shift % LANES
        if shift == 0:
            return value
    return pltpu.roll(value, shift, 1)


def kernel(fields, volume_code, cut_flag, member_bits, result, raw, code, cut, bits, act, kap, inv_count,
           inv_volume, w, acc, hats, xface, yrows, edges, zpack, xzpack, yzpack, cpack,
           rx, ry, re, rz, rxz, ryz, rc, in_sem, send_sem, recv_sem):
    lane8 = lax.broadcasted_iota(jnp.int32, (8, LANES), 1)
    lane1 = lax.broadcasted_iota(jnp.int32, (1, LANES), 1)
    zero8 = jnp.zeros((8, LANES), jnp.float32)

    loads = []
    for index, (source, target) in enumerate(
        ((volume_code, code), (cut_flag, cut), (member_bits, bits), (fields, raw))
    ):
        copy = pltpu.make_async_copy(source, target, in_sem.at[index])
        copy.start()
        loads.append(copy)
    barrier = pltpu.get_barrier_semaphore()
    for travel in TRAVEL:
        pl.semaphore_signal(barrier, inc=1, device_id=neighbour(travel), device_id_type=MESH)

    for x in range(LAYERS):
        for rows in (0, PADDED - 8):
            act[x, rows : rows + 8, :] = jnp.zeros((8, LANES), jnp.int32)
            for f in range(FIELDS + 1):
                w[f, x, rows : rows + 8, :] = zero8
    for copy in loads:
        copy.wait()

    def prepare(t, carry):
        own = pl.ds(pl.multiple_of(8 * t, 8), 8)
        padded = pl.ds(pl.multiple_of(8 * t + 8, 8), 8)
        for x in range(LAYERS):
            kappa = code[x, own, :].astype(jnp.float32) * (1.0 / 1048576.0)
            active = bits[x, own, :] * cut[x, own, :]
            act[x, padded, :] = active
            kap[x, own, :] = kappa
            others = lax.population_count(jnp.bitwise_and(active, ((1 << 27) - 1) ^ (1 << 13)))
            inv_count[x, own, :] = 1.0 / (others + 1).astype(jnp.float32)
            w[FIELDS, x, padded, :] = kappa
            for f in range(FIELDS):
                w[f, x, padded, :] = kappa * raw[f, x, own, :]
        return carry

    lax.fori_loop(0, TILES, prepare, 0)

    def message(stage, sx, sy, sz, chunk):
        count = FIELDS + 1 if stage == 0 else FIELDS
        which = stage // 2
        ix, iy, iz = side(sx), side(sy), side(sz)
        e = 2 * ix + iy
        if sx and not sy and not sz:
            start = chunk * CHUNK
            if stage % 2 == 0:
                source = xface.at[which, ix, 0:count, start : start + CHUNK, :]
                target = rx.at[which, ix, 0:count, start : start + CHUNK, :]
            else:
                mid = hats.at[which, 1]
                source = mid.at[:, 4 if sx == 1 else 1, 8 + start : 8 + start + CHUNK, :]
                target = mid.at[:, 0 if sx == 1 else 5, 8 + start : 8 + start + CHUNK, :]
        elif sy and not sx and not sz:
            source, target = yrows.at[stage, iy], ry.at[stage, iy]
        elif sz and not sx and not sy:
            source, target = zpack.at[stage], rz.at[stage, iz]
        elif sx and sy and not sz:
            source, target = edges.at[stage, e], re.at[stage, e]
        elif sx and sz and not sy:
            source, target = xzpack.at[stage, ix], rxz.at[stage, ix, iz]
        elif sy and sz and not sx:
            source, target = yzpack.at[stage, iy], ryz.at[stage, iy, iz]
        else:
            source, target = cpack.at[stage, e], rc.at[stage, e, iz]
        index = MESSAGES.index((sx, sy, sz, chunk))
        return pltpu.make_async_remote_copy(
            src_ref=source,
            dst_ref=target,
            send_sem=send_sem.at[stage, index],
            recv_sem=recv_sem.at[stage, index],
            device_id=neighbour((sx, sy, sz)),
            device_id_type=MESH,
        )

    def send(stage, chosen):
        for which in MESSAGES:
            if chosen(*which):
                message(stage, *which).start()

    def receive(stage, chosen):
        for which in MESSAGES:
            if chosen(*which):
                message(stage, *which).wait_recv()

    def drain(stage):
        for which in MESSAGES:
            message(stage, *which).wait_send()

    def beside(sx, sy, sz, chunk):
        return sx == 0

    def small(sx, sy, sz, chunk):
        return sx != 0 and (sy != 0 or sz != 0)

    def faces(wanted):
        return lambda sx, sy, sz, chunk: sx != 0 and sy == 0 and sz == 0 and chunk in wanted

    def packed(base, value, p, lane):
        return jnp.where(jnp.right_shift(lane, 1) == p, turn(value, 1 + 2 * p), base)

    def pairs(from_below, from_above, lane):
        return jnp.where(jnp.bitwise_and(lane, 1) == 1, turn(from_below, 1), turn(from_above, -1))

    def placed(pack, p):
        return turn(pack, LANES - 1 - 2 * p)

    def only_ends(value, lane):
        return jnp.where((lane == 0) | (lane == LANES - 1), value, 0.0)

    def pushed(xt, row, dys, count):
        sums = [[None] * count for _ in range(3)]
        for dx in (-1, 0, 1):
            xs = xt - dx
            if xs < 0 or xs >= LAYERS:
                continue
            for dy in dys:
                rows = pl.ds(row - dy, 8)
                active = act[xs, rows, :]
                values = [w[f, xs, rows, :] for f in range(count)]
                for dz in (-1, 0, 1):
                    bit = offset_bit(dx, dy, dz)
                    if bit != 13:
                        chosen = jnp.bitwise_and(active, 1 << bit) != 0
                    for f in range(count):
                        term = values[f] if bit == 13 else jnp.where(chosen, values[f], 0.0)
                        old = sums[dz + 1][f]
                        sums[dz + 1][f] = term if old is None else old + term
        mains, ends = [], []
        for f in range(count):
            up = turn(sums[2][f], 1)
            down = turn(sums[0][f], -1)
            mains.append(
                sums[1][f] + jnp.where(lane8 == 0, 0.0, up) + jnp.where(lane8 == LANES - 1, 0.0, down)
            )
            ends.append(jnp.where(lane8 < LANES // 2, sums[0][f], sums[2][f]))
        return mains, ends

    def scatter(stage, count):
        which = stage // 2
        for sx in SIGNS:
            xt = -1 if sx == -1 else LAYERS
            ix = side(sx)
            pack = zero8
            for t in range(TILES):
                mains, ends = pushed(xt, 8 * t + 8, (-1, 0, 1), count)
                for f in range(count):
                    xface[which, ix, f, 8 * t : 8 * t + 8, :] = mains[f]
                    pack = packed(pack, ends[f], count * t + f, lane8)
            xzpack[stage, ix] = pack
            for sy in SIGNS:
                mains, ends = pushed(xt, 0 if sy == -1 else PADDED - 8, (sy,), count)
                row = 7 if sy == -1 else 0
                e = 2 * ix + side(sy)
                pack = zero8
                for f in range(count):
                    edges[stage, e, f : f + 1, :] = mains[f][row : row + 1, :]
                    pack = packed(pack, ends[f], f, lane8)
                cpack[stage, e] = pack[row : row + 1, :]
        if stage == 0:
            pl.semaphore_wait(barrier, len(TRAVEL))
        send(stage, small)
        send(stage, faces(range(CHUNKS)))

        def rest(t, carry):
            own = pl.ds(pl.multiple_of(8 * t, 8), 8)
            pack = zero8
            for xt in range(LAYERS):
                mains, ends = pushed(xt, 8 * t + 8, (-1, 0, 1), count)
                for f in range(count):
                    acc[f, xt, own, :] = mains[f]
                    pack = packed(pack, ends[f], 4 * f + xt, lane8)
            zpack[stage, t] = pack
            return carry

        lax.fori_loop(0, TILES, rest, 0)
        send(stage, lambda sx, sy, sz, chunk: (sx, sy) == (0, 0))
        for sy in SIGNS:
            row = 7 if sy == -1 else 0
            pack = zero8
            for xt in range(LAYERS):
                mains, ends = pushed(xt, 0 if sy == -1 else PADDED - 8, (sy,), count)
                for f in range(count):
                    p = 4 * f + xt
                    yrows[stage, side(sy), p : p + 1, :] = mains[f][row : row + 1, :]
                    pack = packed(pack, ends[f], p, lane8)
            yzpack[stage, side(sy)] = pack[row : row + 1, :]
        send(stage, lambda sx, sy, sz, chunk: sx == 0 and sy != 0)

    def combine(stage, count):
        odd = stage + 1
        which = stage // 2

        def finish(x, t, sums):
            own = pl.ds(8 * t, 8)
            if stage == 0:
                inverse = 1.0 / sums[FIELDS]
                inv_volume[x, own, :] = inverse
            else:
                inverse = inv_volume[x, own, :]
            for f in range(FIELDS):
                hats[which, 1, f, x + 1, 8 * t + 8 : 8 * t + 16, :] = sums[f] * inverse

        receive(stage, beside)
        for sy in SIGNS:
            iy = side(sy)
            row = 0 if sy == 1 else ROWS - 1
            yz = pairs(ryz[stage, iy, 1], ryz[stage, iy, 0], lane1)
            for x in range(LAYERS):
                for f in range(count):
                    p = 4 * f + x
                    value = ry[stage, iy, p : p + 1, :] + only_ends(placed(yz, p), lane1)
                    acc[f, x, row : row + 1, :] += value
        for t in range(TILES):
            z = pairs(rz[stage, 1, t], rz[stage, 0, t], lane8)
            for x in range(LAYERS):
                sums = []
                for f in range(count):
                    value = acc[f, x, 8 * t : 8 * t + 8, :] + only_ends(placed(z, 4 * f + x), lane8)
                    sums.append(value)
                if x in (0, LAYERS - 1):
                    for f in range(count):
                        acc[f, x, 8 * t : 8 * t + 8, :] = sums[f]
                else:
                    finish(x, t, sums)
        receive(stage, small)
        for sx in SIGNS:
            ix = side(sx)
            x = 0 if sx == 1 else LAYERS - 1
            xz = pairs(rxz[stage, ix, 1], rxz[stage, ix, 0], lane8)
            for t in range(TILES):
                for f in range(count):
                    acc[f, x, 8 * t : 8 * t + 8, :] += only_ends(placed(xz, count * t + f), lane8)
            for sy in SIGNS:
                e = 2 * ix + side(sy)
                row = 0 if sy == 1 else ROWS - 1
                corner = pairs(rc[stage, e, 1], rc[stage, e, 0], lane1)
                for f in range(count):
                    value = re[stage, e, f : f + 1, :] + only_ends(placed(corner, f), lane1)
                    acc[f, x, row : row + 1, :] += value
        for chunk in range(CHUNKS):
            receive(stage, faces((chunk,)))
            for t in range(chunk * CHUNK // 8, (chunk + 1) * CHUNK // 8):
                for sx in SIGNS:
                    x = 0 if sx == 1 else LAYERS - 1
                    sums = []
                    for f in range(count):
                        own = slice(8 * t, 8 * t + 8)
                        sums.append(acc[f, x, own, :] + rx[which, side(sx), f, own, :])
                    finish(x, t, sums)
            send(odd, faces((chunk,)))
        for sx in SIGNS:
            x = 0 if sx == -1 else LAYERS - 1
            pack = zero8
            for t in range(TILES):
                for f in range(FIELDS):
                    value = hats[which, 1, f, x + 1, 8 * t + 8 : 8 * t + 16, :]
                    pack = packed(pack, value, FIELDS * t + f, lane8)
            xzpack[odd, side(sx)] = pack
            for sy in SIGNS:
                row = 8 if sy == -1 else 7 + ROWS
                e = 2 * side(sx) + side(sy)
                pack = jnp.zeros((1, LANES), jnp.float32)
                for f in range(FIELDS):
                    value = hats[which, 1, f, x + 1, row : row + 1, :]
                    edges[odd, e, f : f + 1, :] = value
                    pack = packed(pack, value, f, lane1)
                cpack[odd, e] = pack
        send(odd, small)
        for t in range(TILES):
            pack = zero8
            for x in range(LAYERS):
                for f in range(FIELDS):
                    value = hats[which, 1, f, x + 1, 8 * t + 8 : 8 * t + 16, :]
                    pack = packed(pack, value, 4 * f + x, lane8)
            zpack[odd, t] = pack
        send(odd, lambda sx, sy, sz, chunk: (sx, sy) == (0, 0))
        for sy in SIGNS:
            row = 8 if sy == -1 else 7 + ROWS
            for x in range(LAYERS):
                for f in range(FIELDS):
                    p = 4 * f + x
                    yrows[odd, side(sy), p : p + 1, :] = hats[which, 1, f, x + 1, row : row + 1, :]
            t = 0 if sy == -1 else TILES - 1
            yzpack[odd, side(sy)] = zpack[odd, t, row % 8 : row % 8 + 1, :]
        send(odd, lambda sx, sy, sz, chunk: sx == 0 and sy != 0)
        drain(stage)

    def gather(stage, last):
        which = stage // 2

        def shifted(f, xi, rows, value, ends, lane):
            hats[which, 2, f, xi, rows, :] = jnp.where(lane == LANES - 1, ends, turn(value, -1))
            hats[which, 0, f, xi, rows, :] = jnp.where(lane == 0, ends, turn(value, 1))

        def pulled(sums, x, t, dxs):
            active = act[x, pl.ds(pl.multiple_of(8 * t + 8, 8), 8), :]
            for dx in dxs:
                if sums is None:
                    sums = [hats[which, 1, f, x + 1, pl.ds(8 * t + 8, 8), :] for f in range(FIELDS)]
                for dy in (-1, 0, 1):
                    for dz in (-1, 0, 1):
                        bit = offset_bit(dx, dy, dz)
                        if bit == 13:
                            continue
                        chosen = jnp.bitwise_and(active, 1 << bit) != 0
                        rows = pl.ds(8 * t + 8 + dy, 8)
                        for f in range(FIELDS):
                            value = hats[which, dz + 1, f, x + 1 + dx, rows, :]
                            sums[f] = sums[f] + jnp.where(chosen, value, 0.0)
            return sums

        def finish(x, t, sums):
            own = pl.ds(pl.multiple_of(8 * t, 8), 8)
            scale = inv_count[x, own, :]
            if not last:
                scale = scale * kap[x, own, :]
            for f in range(FIELDS):
                if last:
                    result[f, x, own, :] = sums[f] * scale
                else:
                    w[f, x, pl.ds(pl.multiple_of(8 * t + 8, 8), 8), :] = sums[f] * scale

        receive(stage, beside)
        for sy in SIGNS:
            iy = side(sy)
            row = 7 if sy == 1 else 8 + ROWS
            yz = pairs(ryz[stage, iy, 1], ryz[stage, iy, 0], lane1)
            for x in range(LAYERS):
                for f in range(FIELDS):
                    p = 4 * f + x
                    value = ry[stage, iy, p : p + 1, :]
                    hats[which, 1, f, x + 1, row : row + 1, :] = value
                    shifted(f, x + 1, slice(row, row + 1), value, placed(yz, p), lane1)

        def shifts(t, carry):
            z = pairs(rz[stage, 1, t], rz[stage, 0, t], lane8)
            padded = pl.ds(pl.multiple_of(8 * t + 8, 8), 8)
            for x in range(LAYERS):
                for f in range(FIELDS):
                    value = hats[which, 1, f, x + 1, padded, :]
                    shifted(f, x + 1, padded, value, placed(z, 4 * f + x), lane8)
            return carry

        lax.fori_loop(0, TILES, shifts, 0)

        def interior(t, carry):
            for x in range(LAYERS):
                if x == 0:
                    sums = pulled(None, x, t, (0, 1))
                elif x == LAYERS - 1:
                    sums = pulled(None, x, t, (-1, 0))
                else:
                    finish(x, t, pulled(None, x, t, (-1, 0, 1)))
                    continue
                for f in range(FIELDS):
                    acc[f, x, pl.ds(pl.multiple_of(8 * t, 8), 8), :] = sums[f]
            return carry

        lax.fori_loop(0, TILES, interior, 0)
        receive(stage, lambda sx, sy, sz, chunk: sx != 0)
        for sx in SIGNS:
            ix = side(sx)
            xi = 0 if sx == 1 else LAYERS + 1
            for sy in SIGNS:
                e = 2 * ix + side(sy)
                row = 7 if sy == 1 else 8 + ROWS
                corner = pairs(rc[stage, e, 1], rc[stage, e, 0], lane1)
                for f in range(FIELDS):
                    value = re[stage, e, f : f + 1, :]
                    hats[which, 1, f, xi, row : row + 1, :] = value
                    shifted(f, xi, slice(row, row + 1), value, placed(corner, f), lane1)
            xz = pairs(rxz[stage, ix, 1], rxz[stage, ix, 0], lane8)
            for t in range(TILES):
                rows = slice(8 * t + 8, 8 * t + 16)
                for f in range(FIELDS):
                    shifted(f, xi, rows, hats[which, 1, f, xi, rows, :], placed(xz, FIELDS * t + f), lane8)

        def boundary(t, carry):
            for x, dx in ((0, -1), (LAYERS - 1, 1)):
                sums = [acc[f, x, pl.ds(pl.multiple_of(8 * t, 8), 8), :] for f in range(FIELDS)]
                finish(x, t, pulled(sums, x, t, (dx,)))
            return carry

        lax.fori_loop(0, TILES, boundary, 0, unroll=4)

    scatter(0, FIELDS + 1)
    combine(0, FIELDS + 1)
    gather(1, False)
    scatter(2, FIELDS)
    drain(1)
    combine(2, FIELDS)
    gather(3, True)
    drain(3)


def body(fields, volume_code, cut_flag, member_bits):
    f32, i32 = jnp.float32, jnp.int32
    vmem = pltpu.VMEM
    block = (LAYERS, ROWS, LANES)
    padded = (LAYERS, PADDED, LANES)
    row_count = 24
    scratch = [
        vmem((FIELDS,) + block, f32),
        vmem(block, i32),
        vmem(block, i32),
        vmem(block, i32),
        vmem(padded, i32),
        vmem(block, f32),
        vmem(block, f32),
        vmem(block, f32),
        vmem((FIELDS + 1,) + padded, f32),
        vmem((FIELDS + 1,) + block, f32),
        vmem((2, 3, FIELDS, LAYERS + 2, PADDED, LANES), f32),
        vmem((2, 2, FIELDS + 1, ROWS, LANES), f32),
        vmem((4, 2, row_count, LANES), f32),
        vmem((4, 4, 8, LANES), f32),
        vmem((4, TILES, 8, LANES), f32),
        vmem((4, 2, 8, LANES), f32),
        vmem((4, 2, 1, LANES), f32),
        vmem((4, 4, 1, LANES), f32),
        vmem((2, 2, FIELDS + 1, ROWS, LANES), f32),
        vmem((4, 2, row_count, LANES), f32),
        vmem((4, 4, 8, LANES), f32),
        vmem((4, 2, TILES, 8, LANES), f32),
        vmem((4, 2, 2, 8, LANES), f32),
        vmem((4, 2, 2, 1, LANES), f32),
        vmem((4, 4, 2, 1, LANES), f32),
        pltpu.SemaphoreType.DMA((4,)),
        pltpu.SemaphoreType.DMA((4, len(MESSAGES))),
        pltpu.SemaphoreType.DMA((4, len(MESSAGES))),
    ]
    in_hbm = pl.BlockSpec(memory_space=pltpu.MemorySpace.HBM)
    in_vmem = pl.BlockSpec(memory_space=pltpu.MemorySpace.VMEM)
    return pl.pallas_call(
        kernel,
        out_shape=jax.ShapeDtypeStruct((FIELDS,) + block, f32),
        in_specs=[in_hbm] * 4,
        out_specs=in_vmem,
        scratch_shapes=scratch,
        compiler_params=pltpu.CompilerParams(
            collective_id=0, has_side_effects=True, vmem_limit_bytes=67043328
        ),
    )(fields, volume_code, cut_flag, member_bits)


def solution(mesh):
    in_specs = (
        P(None, "gx", "gy", "gz"),
        P("gx", "gy", "gz"),
        P("gx", "gy", "gz"),
        P("gx", "gy", "gz"),
    )
    out_specs = P(None, "gx", "gy", "gz")
    return jax.shard_map(body, mesh=mesh, in_specs=in_specs, out_specs=out_specs, check_vma=False)
```

```python
import jax
import jax.numpy as jnp
from jax import lax
from jax.experimental import pallas as pl
from jax.experimental.pallas import tpu as pltpu
from jax.sharding import PartitionSpec as P

MESH = pl.DeviceIdType.MESH
FIELDS = 4
LAYERS = 4
ROWS = 64
TILES = ROWS // 8
PADDED = ROWS + 16
LANES = 128
CHUNK = 16
CHUNKS = ROWS // CHUNK
ORDER = (0, CHUNKS - 1) + tuple(range(1, CHUNKS - 1))
ROW_COUNT = 24
SIGNS = (-1, 1)

TRAVEL = []
for kind in ((1, 0, 0), (1, 1, 0), (1, 0, 1), (1, 1, 1), (0, 0, 1), (0, 1, 0), (0, 1, 1)):
    for sx in SIGNS if kind[0] else (0,):
        for sy in SIGNS if kind[1] else (0,):
            for sz in SIGNS if kind[2] else (0,):
                TRAVEL.append((sx, sy, sz))
MESSAGES = []
for travel in TRAVEL:
    for chunk in range(CHUNKS if travel[1:] == (0, 0) else 1):
        MESSAGES.append(travel + (chunk,))


def side(sign):
    return (sign + 1) // 2


def offset_bit(dx, dy, dz):
    return 9 * (dx + 1) + 3 * (dy + 1) + (dz + 1)


def neighbour(travel):
    result = {}
    for axis, sign in zip(("gx", "gy", "gz"), travel):
        if sign:
            count = lax.axis_size(axis)
            result[axis] = lax.rem(lax.axis_index(axis) + sign + count, count)
    return result


def turn(value, shift):
    if isinstance(shift, int):
        shift = shift % LANES
        if shift == 0:
            return value
    return pltpu.roll(value, shift, 1)


def kernel(fields, volume_code, cut_flag, member_bits, result, raw, code, cut, bits, act, kap, inv_count,
           inv_volume, w, acc, hats, xface, yrows, edges, zpack, xzpack, yzpack, cpack,
           rx, ry, re, rz, rxz, ryz, rc, in_sem, send_sem, recv_sem, lengths):
    lane8 = lax.broadcasted_iota(jnp.int32, (8, LANES), 1)
    lane1 = lax.broadcasted_iota(jnp.int32, (1, LANES), 1)
    zero8 = jnp.zeros((8, LANES), jnp.float32)

    loads = []
    for index, (source, target) in enumerate(
        ((volume_code, code), (cut_flag, cut), (member_bits, bits), (fields, raw))
    ):
        copy = pltpu.make_async_copy(source, target, in_sem.at[index])
        copy.start()
        loads.append(copy)
    barrier = pltpu.get_barrier_semaphore()
    for travel in TRAVEL:
        pl.semaphore_signal(barrier, inc=1, device_id=neighbour(travel), device_id_type=MESH)

    for x in range(LAYERS):
        for rows in (0, PADDED - 8):
            act[x, rows : rows + 8, :] = jnp.zeros((8, LANES), jnp.int32)
            for f in range(FIELDS + 1):
                w[f, x, rows : rows + 8, :] = zero8
    for copy in loads:
        copy.wait()

    def prepare(t, carry):
        own = pl.ds(pl.multiple_of(8 * t, 8), 8)
        padded = pl.ds(pl.multiple_of(8 * t + 8, 8), 8)
        for x in range(LAYERS):
            kappa = code[x, own, :].astype(jnp.float32) * (1.0 / 1048576.0)
            active = bits[x, own, :] * cut[x, own, :]
            act[x, padded, :] = active
            kap[x, own, :] = kappa
            others = lax.population_count(jnp.bitwise_and(active, ((1 << 27) - 1) ^ (1 << 13)))
            inv_count[x, own, :] = 1.0 / (others + 1).astype(jnp.float32)
            w[FIELDS, x, padded, :] = kappa
            for f in range(FIELDS):
                w[f, x, padded, :] = kappa * raw[f, x, own, :]
        return carry

    lax.fori_loop(0, TILES, prepare, 0)

    def message(stage, sx, sy, sz, chunk):
        count = FIELDS + 1 if stage == 0 else FIELDS
        which = stage // 2
        ix, iy, iz = side(sx), side(sy), side(sz)
        e = 2 * ix + iy
        if sx and not sy and not sz:
            start = chunk * CHUNK
            if stage % 2 == 0:
                source = xface.at[which, ix, 0:count, start : start + CHUNK, :]
                target = rx.at[which, ix, 0:count, start : start + CHUNK, :]
            else:
                mid = hats.at[which, 1]
                source = mid.at[:, 4 if sx == 1 else 1, 8 + start : 8 + start + CHUNK, :]
                target = mid.at[:, 0 if sx == 1 else 5, 8 + start : 8 + start + CHUNK, :]
        elif sy and not sx and not sz:
            source, target = yrows.at[stage, iy], ry.at[stage, iy]
        elif sz and not sx and not sy:
            source, target = zpack.at[stage], rz.at[stage, iz]
        elif sx and sy and not sz:
            source, target = edges.at[stage, e], re.at[stage, e]
        elif sx and sz and not sy:
            source, target = xzpack.at[stage, ix], rxz.at[stage, ix, iz]
        elif sy and sz and not sx:
            source, target = yzpack.at[stage, iy], ryz.at[stage, iy, iz]
        else:
            source, target = cpack.at[stage, e], rc.at[stage, e, iz]
        group = 0 if sx == 0 else 1 if sy or sz else 2 + chunk
        return pltpu.make_async_remote_copy(
            src_ref=source,
            dst_ref=target,
            send_sem=send_sem.at[stage],
            recv_sem=recv_sem.at[stage, group],
            device_id=neighbour((sx, sy, sz)),
            device_id_type=MESH,
        )

    def send(stage, chosen):
        for which in MESSAGES:
            if chosen(*which):
                message(stage, *which).start()

    def rows_of(stage, which):
        sx, sy, sz, chunk = which
        if (sy, sz) == (0, 0):
            return CHUNK * (FIELDS + 1 if stage == 0 else FIELDS)
        if (sx, sz) == (0, 0):
            return ROW_COUNT
        if (sx, sy) == (0, 0):
            return ROWS
        return 8 if sx and not (sy and sz) else 1

    def await_rows(semaphore, rows):
        part = lengths.at[0:rows]
        pltpu.make_async_copy(part, part, semaphore).wait()

    def receive(stage, group):
        chosen = [beside, small, None][min(group, 2)] or faces((group - 2,))
        rows = sum(rows_of(stage, which) for which in MESSAGES if chosen(*which))
        await_rows(recv_sem.at[stage, group], rows)

    def drain(stage):
        await_rows(send_sem.at[stage], sum(rows_of(stage, which) for which in MESSAGES))

    def beside(sx, sy, sz, chunk):
        return sx == 0

    def small(sx, sy, sz, chunk):
        return sx != 0 and (sy != 0 or sz != 0)

    def faces(wanted):
        return lambda sx, sy, sz, chunk: sx != 0 and sy == 0 and sz == 0 and chunk in wanted

    def packed(base, value, p, lane):
        return jnp.where(jnp.right_shift(lane, 1) == p, turn(value, 1 + 2 * p), base)

    def pairs(from_below, from_above, lane):
        return jnp.where(jnp.bitwise_and(lane, 1) == 1, turn(from_below, 1), turn(from_above, -1))

    def placed(pack, p):
        return turn(pack, LANES - 1 - 2 * p)

    def only_ends(value, lane):
        return jnp.where((lane == 0) | (lane == LANES - 1), value, 0.0)

    def pushed(xt, row, dys, count):
        sums = [[None] * count for _ in range(3)]
        for dx in (-1, 0, 1):
            xs = xt - dx
            if xs < 0 or xs >= LAYERS:
                continue
            for dy in dys:
                rows = pl.ds(row - dy, 8)
                active = act[xs, rows, :]
                values = [w[f, xs, rows, :] for f in range(count)]
                for dz in (-1, 0, 1):
                    bit = offset_bit(dx, dy, dz)
                    if bit != 13:
                        chosen = jnp.bitwise_and(active, 1 << bit) != 0
                    for f in range(count):
                        term = values[f] if bit == 13 else jnp.where(chosen, values[f], 0.0)
                        old = sums[dz + 1][f]
                        sums[dz + 1][f] = term if old is None else old + term
        mains, ends = [], []
        for f in range(count):
            up = turn(sums[2][f], 1)
            down = turn(sums[0][f], -1)
            mains.append(
                sums[1][f] + jnp.where(lane8 == 0, 0.0, up) + jnp.where(lane8 == LANES - 1, 0.0, down)
            )
            ends.append(jnp.where(lane8 < LANES // 2, sums[0][f], sums[2][f]))
        return mains, ends

    def scatter(stage, count):
        which = stage // 2
        for sx in SIGNS:
            xt = -1 if sx == -1 else LAYERS
            ix = side(sx)
            for sy in SIGNS:
                mains, ends = pushed(xt, 0 if sy == -1 else PADDED - 8, (sy,), count)
                row = 7 if sy == -1 else 0
                e = 2 * ix + side(sy)
                pack = zero8
                for f in range(count):
                    edges[stage, e, f : f + 1, :] = mains[f][row : row + 1, :]
                    pack = packed(pack, ends[f], f, lane8)
                cpack[stage, e] = pack[row : row + 1, :]
        if stage == 0:
            pl.semaphore_wait(barrier, len(TRAVEL))
        send(stage, lambda sx, sy, sz, chunk: sx != 0 and sy != 0)
        for sx in SIGNS:
            xt = -1 if sx == -1 else LAYERS
            ix = side(sx)
            pack = zero8
            for t in range(TILES):
                mains, ends = pushed(xt, 8 * t + 8, (-1, 0, 1), count)
                for f in range(count):
                    xface[which, ix, f, 8 * t : 8 * t + 8, :] = mains[f]
                    pack = packed(pack, ends[f], count * t + f, lane8)
            xzpack[stage, ix] = pack
        send(stage, lambda sx, sy, sz, chunk: sx != 0 and sy == 0 and sz != 0)
        for chunk in ORDER:
            send(stage, faces((chunk,)))

        def rest(t, carry):
            own = pl.ds(pl.multiple_of(8 * t, 8), 8)
            pack = zero8
            for xt in range(LAYERS):
                mains, ends = pushed(xt, 8 * t + 8, (-1, 0, 1), count)
                for f in range(count):
                    acc[f, xt, own, :] = mains[f]
                    pack = packed(pack, ends[f], 4 * f + xt, lane8)
            zpack[stage, t] = pack
            return carry

        lax.fori_loop(0, TILES, rest, 0)
        send(stage, lambda sx, sy, sz, chunk: (sx, sy) == (0, 0))
        for sy in SIGNS:
            row = 7 if sy == -1 else 0
            pack = zero8
            for xt in range(LAYERS):
                mains, ends = pushed(xt, 0 if sy == -1 else PADDED - 8, (sy,), count)
                for f in range(count):
                    p = 4 * f + xt
                    yrows[stage, side(sy), p : p + 1, :] = mains[f][row : row + 1, :]
                    pack = packed(pack, ends[f], p, lane8)
            yzpack[stage, side(sy)] = pack[row : row + 1, :]
        send(stage, lambda sx, sy, sz, chunk: sx == 0 and sy != 0)

    def combine(stage, count):
        odd = stage + 1
        which = stage // 2

        def finish(x, t, sums):
            own = pl.ds(8 * t, 8)
            if stage == 0:
                inverse = 1.0 / sums[FIELDS]
                inv_volume[x, own, :] = inverse
            else:
                inverse = inv_volume[x, own, :]
            for f in range(FIELDS):
                hats[which, 1, f, x + 1, 8 * t + 8 : 8 * t + 16, :] = sums[f] * inverse

        receive(stage, 0)
        for sy in SIGNS:
            iy = side(sy)
            row = 0 if sy == 1 else ROWS - 1
            yz = pairs(ryz[stage, iy, 1], ryz[stage, iy, 0], lane1)
            for x in range(LAYERS):
                for f in range(count):
                    p = 4 * f + x
                    value = ry[stage, iy, p : p + 1, :] + only_ends(placed(yz, p), lane1)
                    acc[f, x, row : row + 1, :] += value
        for t in range(TILES):
            z = pairs(rz[stage, 1, t], rz[stage, 0, t], lane8)
            for x in range(LAYERS):
                sums = []
                for f in range(count):
                    value = acc[f, x, 8 * t : 8 * t + 8, :] + only_ends(placed(z, 4 * f + x), lane8)
                    sums.append(value)
                if x in (0, LAYERS - 1):
                    for f in range(count):
                        acc[f, x, 8 * t : 8 * t + 8, :] = sums[f]
                else:
                    finish(x, t, sums)
        receive(stage, 1)
        for sx in SIGNS:
            ix = side(sx)
            x = 0 if sx == 1 else LAYERS - 1
            xz = pairs(rxz[stage, ix, 1], rxz[stage, ix, 0], lane8)
            for t in range(TILES):
                for f in range(count):
                    acc[f, x, 8 * t : 8 * t + 8, :] += only_ends(placed(xz, count * t + f), lane8)
            for sy in SIGNS:
                e = 2 * ix + side(sy)
                row = 0 if sy == 1 else ROWS - 1
                corner = pairs(rc[stage, e, 1], rc[stage, e, 0], lane1)
                for f in range(count):
                    value = re[stage, e, f : f + 1, :] + only_ends(placed(corner, f), lane1)
                    acc[f, x, row : row + 1, :] += value
        for position, chunk in enumerate(ORDER):
            receive(stage, 2 + chunk)
            for t in range(chunk * CHUNK // 8, (chunk + 1) * CHUNK // 8):
                for sx in SIGNS:
                    x = 0 if sx == 1 else LAYERS - 1
                    sums = []
                    for f in range(count):
                        own = slice(8 * t, 8 * t + 8)
                        sums.append(acc[f, x, own, :] + rx[which, side(sx), f, own, :])
                    finish(x, t, sums)
            if position == 1:
                for sx in SIGNS:
                    x = 0 if sx == -1 else LAYERS - 1
                    for sy in SIGNS:
                        row = 8 if sy == -1 else 7 + ROWS
                        e = 2 * side(sx) + side(sy)
                        pack = jnp.zeros((1, LANES), jnp.float32)
                        for f in range(FIELDS):
                            value = hats[which, 1, f, x + 1, row : row + 1, :]
                            edges[odd, e, f : f + 1, :] = value
                            pack = packed(pack, value, f, lane1)
                        cpack[odd, e] = pack
                send(odd, lambda sx, sy, sz, chunk: sx != 0 and sy != 0)
            if position == CHUNKS - 1:
                for sx in SIGNS:
                    x = 0 if sx == -1 else LAYERS - 1
                    pack = zero8
                    for t in range(TILES):
                        for f in range(FIELDS):
                            value = hats[which, 1, f, x + 1, 8 * t + 8 : 8 * t + 16, :]
                            pack = packed(pack, value, FIELDS * t + f, lane8)
                    xzpack[odd, side(sx)] = pack
                send(odd, lambda sx, sy, sz, chunk: sx != 0 and sy == 0 and sz != 0)
            send(odd, faces((chunk,)))
        for t in range(TILES):
            pack = zero8
            for x in range(LAYERS):
                for f in range(FIELDS):
                    value = hats[which, 1, f, x + 1, 8 * t + 8 : 8 * t + 16, :]
                    pack = packed(pack, value, 4 * f + x, lane8)
            zpack[odd, t] = pack
        send(odd, lambda sx, sy, sz, chunk: (sx, sy) == (0, 0))
        for sy in SIGNS:
            row = 8 if sy == -1 else 7 + ROWS
            for x in range(LAYERS):
                for f in range(FIELDS):
                    p = 4 * f + x
                    yrows[odd, side(sy), p : p + 1, :] = hats[which, 1, f, x + 1, row : row + 1, :]
            t = 0 if sy == -1 else TILES - 1
            yzpack[odd, side(sy)] = zpack[odd, t, row % 8 : row % 8 + 1, :]
        send(odd, lambda sx, sy, sz, chunk: sx == 0 and sy != 0)
        drain(stage)

    def gather(stage, last):
        which = stage // 2

        def shifted(f, xi, rows, value, ends, lane):
            hats[which, 2, f, xi, rows, :] = jnp.where(lane == LANES - 1, ends, turn(value, -1))
            hats[which, 0, f, xi, rows, :] = jnp.where(lane == 0, ends, turn(value, 1))

        def pulled(sums, x, t, dxs):
            active = act[x, pl.ds(pl.multiple_of(8 * t + 8, 8), 8), :]
            for dx in dxs:
                if sums is None:
                    sums = [hats[which, 1, f, x + 1, pl.ds(8 * t + 8, 8), :] for f in range(FIELDS)]
                for dy in (-1, 0, 1):
                    for dz in (-1, 0, 1):
                        bit = offset_bit(dx, dy, dz)
                        if bit == 13:
                            continue
                        chosen = jnp.bitwise_and(active, 1 << bit) != 0
                        rows = pl.ds(8 * t + 8 + dy, 8)
                        for f in range(FIELDS):
                            value = hats[which, dz + 1, f, x + 1 + dx, rows, :]
                            sums[f] = sums[f] + jnp.where(chosen, value, 0.0)
            return sums

        def finish(x, t, sums):
            own = pl.ds(pl.multiple_of(8 * t, 8), 8)
            scale = inv_count[x, own, :]
            if not last:
                scale = scale * kap[x, own, :]
            for f in range(FIELDS):
                if last:
                    result[f, x, own, :] = sums[f] * scale
                else:
                    w[f, x, pl.ds(pl.multiple_of(8 * t + 8, 8), 8), :] = sums[f] * scale

        def rotations(t, carry):
            padded = pl.ds(pl.multiple_of(8 * t + 8, 8), 8)
            for x in range(LAYERS):
                for f in range(FIELDS):
                    value = hats[which, 1, f, x + 1, padded, :]
                    hats[which, 2, f, x + 1, padded, :] = turn(value, -1)
                    hats[which, 0, f, x + 1, padded, :] = turn(value, 1)
            return carry

        lax.fori_loop(0, TILES, rotations, 0)
        receive(stage, 0)
        for sy in SIGNS:
            iy = side(sy)
            row = 7 if sy == 1 else 8 + ROWS
            yz = pairs(ryz[stage, iy, 1], ryz[stage, iy, 0], lane1)
            for x in range(LAYERS):
                for f in range(FIELDS):
                    p = 4 * f + x
                    value = ry[stage, iy, p : p + 1, :]
                    hats[which, 1, f, x + 1, row : row + 1, :] = value
                    shifted(f, x + 1, slice(row, row + 1), value, placed(yz, p), lane1)

        def new_ends(t, carry):
            z = pairs(rz[stage, 1, t], rz[stage, 0, t], lane8)
            padded = pl.ds(pl.multiple_of(8 * t + 8, 8), 8)
            for x in range(LAYERS):
                for f in range(FIELDS):
                    ends = placed(z, 4 * f + x)
                    for k, lane in ((2, LANES - 1), (0, 0)):
                        old = hats[which, k, f, x + 1, padded, :]
                        hats[which, k, f, x + 1, padded, :] = jnp.where(lane8 == lane, ends, old)
            return carry

        lax.fori_loop(0, TILES, new_ends, 0)

        def interior(t, carry):
            for x in range(LAYERS):
                if x == 0:
                    sums = pulled(None, x, t, (0, 1))
                elif x == LAYERS - 1:
                    sums = pulled(None, x, t, (-1, 0))
                else:
                    finish(x, t, pulled(None, x, t, (-1, 0, 1)))
                    continue
                for f in range(FIELDS):
                    acc[f, x, pl.ds(pl.multiple_of(8 * t, 8), 8), :] = sums[f]
            return carry

        lax.fori_loop(0, TILES, interior, 0)
        drain(stage)
        for group in range(1, 2 + CHUNKS):
            receive(stage, group)
        for sx in SIGNS:
            ix = side(sx)
            xi = 0 if sx == 1 else LAYERS + 1
            for sy in SIGNS:
                e = 2 * ix + side(sy)
                row = 7 if sy == 1 else 8 + ROWS
                corner = pairs(rc[stage, e, 1], rc[stage, e, 0], lane1)
                for f in range(FIELDS):
                    value = re[stage, e, f : f + 1, :]
                    hats[which, 1, f, xi, row : row + 1, :] = value
                    shifted(f, xi, slice(row, row + 1), value, placed(corner, f), lane1)
            xz = pairs(rxz[stage, ix, 1], rxz[stage, ix, 0], lane8)
            for t in range(TILES):
                rows = slice(8 * t + 8, 8 * t + 16)
                for f in range(FIELDS):
                    shifted(f, xi, rows, hats[which, 1, f, xi, rows, :], placed(xz, FIELDS * t + f), lane8)

        def boundary(t, carry):
            for x, dx in ((0, -1), (LAYERS - 1, 1)):
                sums = [acc[f, x, pl.ds(pl.multiple_of(8 * t, 8), 8), :] for f in range(FIELDS)]
                finish(x, t, pulled(sums, x, t, (dx,)))
            return carry

        lax.fori_loop(0, TILES, boundary, 0, unroll=4)

    scatter(0, FIELDS + 1)
    combine(0, FIELDS + 1)
    gather(1, False)
    scatter(2, FIELDS)
    combine(2, FIELDS)
    gather(3, True)


def body(fields, volume_code, cut_flag, member_bits):
    f32, i32 = jnp.float32, jnp.int32
    vmem = pltpu.VMEM
    block = (LAYERS, ROWS, LANES)
    padded = (LAYERS, PADDED, LANES)
    scratch = [
        vmem((FIELDS,) + block, f32),
        vmem(block, i32),
        vmem(block, i32),
        vmem(block, i32),
        vmem(padded, i32),
        vmem(block, f32),
        vmem(block, f32),
        vmem(block, f32),
        vmem((FIELDS + 1,) + padded, f32),
        vmem((FIELDS + 1,) + block, f32),
        vmem((2, 3, FIELDS, LAYERS + 2, PADDED, LANES), f32),
        vmem((2, 2, FIELDS + 1, ROWS, LANES), f32),
        vmem((4, 2, ROW_COUNT, LANES), f32),
        vmem((4, 4, 8, LANES), f32),
        vmem((4, TILES, 8, LANES), f32),
        vmem((4, 2, 8, LANES), f32),
        vmem((4, 2, 1, LANES), f32),
        vmem((4, 4, 1, LANES), f32),
        vmem((2, 2, FIELDS + 1, ROWS, LANES), f32),
        vmem((4, 2, ROW_COUNT, LANES), f32),
        vmem((4, 4, 8, LANES), f32),
        vmem((4, 2, TILES, 8, LANES), f32),
        vmem((4, 2, 2, 8, LANES), f32),
        vmem((4, 2, 2, 1, LANES), f32),
        vmem((4, 4, 2, 1, LANES), f32),
        pltpu.SemaphoreType.DMA((4,)),
        pltpu.SemaphoreType.DMA((4,)),
        pltpu.SemaphoreType.DMA((4, 2 + CHUNKS)),
        vmem((1024, 1, LANES), f32),
    ]
    in_hbm = pl.BlockSpec(memory_space=pltpu.MemorySpace.HBM)
    in_vmem = pl.BlockSpec(memory_space=pltpu.MemorySpace.VMEM)
    operands = (fields, volume_code, cut_flag, member_bits)
    return pl.pallas_call(
        kernel,
        out_shape=jax.ShapeDtypeStruct((FIELDS,) + block, f32),
        in_specs=[in_hbm] * 4,
        out_specs=in_vmem,
        scratch_shapes=scratch,
        compiler_params=pltpu.CompilerParams(
            collective_id=0, has_side_effects=True, vmem_limit_bytes=52000000
        ),
    )(*[pltpu.with_memory_space_constraint(a, pltpu.MemorySpace.HBM) for a in operands])


def solution(mesh):
    in_specs = (
        P(None, "gx", "gy", "gz"),
        P("gx", "gy", "gz"),
        P("gx", "gy", "gz"),
        P("gx", "gy", "gz"),
    )
    out_specs = P(None, "gx", "gy", "gz")
    return jax.shard_map(body, mesh=mesh, in_specs=in_specs, out_specs=out_specs, check_vma=False)
```

```python
import jax
import jax.numpy as jnp
from jax import lax
from jax.experimental import pallas as pl
from jax.experimental.pallas import tpu as pltpu
from jax.sharding import PartitionSpec as P

MESH = pl.DeviceIdType.MESH
FIELDS = 4
LAYERS = 4
ROWS = 64
TILES = ROWS // 8
PADDED = ROWS + 16
LANES = 128
CHUNK = 16
CHUNKS = ROWS // CHUNK
ORDER = (0, CHUNKS - 1) + tuple(range(1, CHUNKS - 1))
ROW_COUNT = 24
SIGNS = (-1, 1)

TRAVEL = []
for kind in ((1, 0, 0), (1, 1, 0), (1, 0, 1), (1, 1, 1), (0, 0, 1), (0, 1, 0), (0, 1, 1)):
    for sx in SIGNS if kind[0] else (0,):
        for sy in SIGNS if kind[1] else (0,):
            for sz in SIGNS if kind[2] else (0,):
                TRAVEL.append((sx, sy, sz))
MESSAGES = []
for travel in TRAVEL:
    for chunk in range(CHUNKS if travel[1:] == (0, 0) else 1):
        MESSAGES.append(travel + (chunk,))


def side(sign):
    return (sign + 1) // 2


def offset_bit(dx, dy, dz):
    return 9 * (dx + 1) + 3 * (dy + 1) + (dz + 1)


def neighbour(travel):
    result = {}
    for axis, sign in zip(("gx", "gy", "gz"), travel):
        if sign:
            count = lax.axis_size(axis)
            result[axis] = lax.rem(lax.axis_index(axis) + sign + count, count)
    return result


def bits_of(dx=None, dy=None, dz=None):
    result = 0
    for x in (-1, 0, 1):
        for y in (-1, 0, 1):
            for z in (-1, 0, 1):
                if dx in (None, x) and dy in (None, y) and dz in (None, z):
                    result |= 1 << offset_bit(x, y, z)
    return result


def turn(value, shift):
    if isinstance(shift, int):
        shift = shift % LANES
        if shift == 0:
            return value
    return pltpu.roll(value, shift, 1)


def kernel(fields, volume_code, cut_flag, member_bits, result, raw, code, cut, bits, act, kap, inv_count,
           inv_volume, w, acc, hats, xface, yrows, edges, zpack, xzpack, yzpack, cpack,
           rx, ry, re, rz, rxz, ryz, rc, in_sem, send_sem, recv_sem, lengths, inner, ends_act, beyond):
    lane8 = lax.broadcasted_iota(jnp.int32, (8, LANES), 1)
    lane1 = lax.broadcasted_iota(jnp.int32, (1, LANES), 1)
    zero8 = jnp.zeros((8, LANES), jnp.float32)

    loads = []
    for index, (source, target) in enumerate(
        ((volume_code, code), (cut_flag, cut), (member_bits, bits), (fields, raw))
    ):
        copy = pltpu.make_async_copy(source, target, in_sem.at[index])
        copy.start()
        loads.append(copy)
    barrier = pltpu.get_barrier_semaphore()
    for travel in TRAVEL:
        pl.semaphore_signal(barrier, inc=1, device_id=neighbour(travel), device_id_type=MESH)

    for x in range(LAYERS):
        for rows in (0, PADDED - 8):
            act[x, rows : rows + 8, :] = jnp.zeros((8, LANES), jnp.int32)
            beyond[rows : rows + 8, :] = zero8
            for f in range(FIELDS + 1):
                w[f, x, rows : rows + 8, :] = zero8
    for copy in loads:
        copy.wait()

    def prepare(t, carry):
        own = pl.ds(pl.multiple_of(8 * t, 8), 8)
        padded = pl.ds(pl.multiple_of(8 * t + 8, 8), 8)
        for x in range(LAYERS):
            kappa = code[x, own, :].astype(jnp.float32) * (1.0 / 1048576.0)
            active = bits[x, own, :] * cut[x, own, :]
            act[x, padded, :] = active
            kap[x, own, :] = kappa
            others = lax.population_count(jnp.bitwise_and(active, ((1 << 27) - 1) ^ (1 << 13)))
            inv_count[x, own, :] = 1.0 / (others + 1).astype(jnp.float32)
            w[FIELDS, x, padded, :] = kappa
            for f in range(FIELDS):
                w[f, x, padded, :] = kappa * raw[f, x, own, :]
        return carry

    lax.fori_loop(0, TILES, prepare, 0)

    def message(stage, sx, sy, sz, chunk):
        count = FIELDS + 1 if stage == 0 else FIELDS
        which = stage // 2
        ix, iy, iz = side(sx), side(sy), side(sz)
        e = 2 * ix + iy
        if sx and not sy and not sz:
            start = chunk * CHUNK
            if stage % 2 == 0:
                source = xface.at[which, ix, 0:count, start : start + CHUNK, :]
                target = rx.at[which, ix, 0:count, start : start + CHUNK, :]
            else:
                mid = hats.at[which, 1]
                source = mid.at[:, 4 if sx == 1 else 1, 8 + start : 8 + start + CHUNK, :]
                target = mid.at[:, 0 if sx == 1 else 5, 8 + start : 8 + start + CHUNK, :]
        elif sy and not sx and not sz:
            source, target = yrows.at[stage, iy], ry.at[stage, iy]
        elif sz and not sx and not sy:
            source, target = zpack.at[stage], rz.at[stage, iz]
        elif sx and sy and not sz:
            source, target = edges.at[stage, e], re.at[stage, e]
        elif sx and sz and not sy:
            source, target = xzpack.at[stage, ix], rxz.at[stage, ix, iz]
        elif sy and sz and not sx:
            source, target = yzpack.at[stage, iy], ryz.at[stage, iy, iz]
        else:
            source, target = cpack.at[stage, e], rc.at[stage, e, iz]
        group = 0 if sx == 0 else 1 if sy or sz else 2 + chunk
        return pltpu.make_async_remote_copy(
            src_ref=source,
            dst_ref=target,
            send_sem=send_sem.at[stage],
            recv_sem=recv_sem.at[stage, group],
            device_id=neighbour((sx, sy, sz)),
            device_id_type=MESH,
        )

    def send(stage, chosen):
        for which in MESSAGES:
            if chosen(*which):
                message(stage, *which).start()

    def rows_of(stage, which):
        sx, sy, sz, chunk = which
        if (sy, sz) == (0, 0):
            return CHUNK * (FIELDS + 1 if stage == 0 else FIELDS)
        if (sx, sz) == (0, 0):
            return ROW_COUNT
        if (sx, sy) == (0, 0):
            return ROWS // 2
        return 8 if sx and not (sy and sz) else 1

    def await_rows(semaphore, rows):
        part = lengths.at[0:rows]
        pltpu.make_async_copy(part, part, semaphore).wait()

    def receive(stage, group):
        chosen = [beside, small, None][min(group, 2)] or faces((group - 2,))
        rows = sum(rows_of(stage, which) for which in MESSAGES if chosen(*which))
        await_rows(recv_sem.at[stage, group], rows)

    def drain(stage):
        await_rows(send_sem.at[stage], sum(rows_of(stage, which) for which in MESSAGES))

    def beside(sx, sy, sz, chunk):
        return sx == 0

    def small(sx, sy, sz, chunk):
        return sx != 0 and (sy != 0 or sz != 0)

    def faces(wanted):
        return lambda sx, sy, sz, chunk: sx != 0 and sy == 0 and sz == 0 and chunk in wanted

    def packed(base, value, p, lane):
        return jnp.where(jnp.right_shift(lane, 1) == p, turn(value, 1 + 2 * p), base)

    def pairs(from_below, from_above, lane):
        return jnp.where(jnp.bitwise_and(lane, 1) == 1, turn(from_below, 1), turn(from_above, -1))

    def placed(pack, p):
        return turn(pack, LANES - 1 - 2 * p)

    def only_ends(value, lane):
        return jnp.where((lane == 0) | (lane == LANES - 1), value, 0.0)

    def pushed(xt, row, dys, count):
        sums = [[None] * count for _ in range(3)]
        for dx in (-1, 0, 1):
            xs = xt - dx
            if xs < 0 or xs >= LAYERS:
                continue
            for dy in dys:
                rows = pl.ds(row - dy, 8)
                active = act[xs, rows, :]
                values = [w[f, xs, rows, :] for f in range(count)]
                for dz in (-1, 0, 1):
                    bit = offset_bit(dx, dy, dz)
                    if bit != 13:
                        chosen = jnp.bitwise_and(active, 1 << bit) != 0
                    for f in range(count):
                        term = values[f] if bit == 13 else jnp.where(chosen, values[f], 0.0)
                        old = sums[dz + 1][f]
                        sums[dz + 1][f] = term if old is None else old + term
        mains, ends = [], []
        for f in range(count):
            up = turn(sums[2][f], 1)
            down = turn(sums[0][f], -1)
            mains.append(
                sums[1][f] + jnp.where(lane8 == 0, 0.0, up) + jnp.where(lane8 == LANES - 1, 0.0, down)
            )
            ends.append(jnp.where(lane8 < LANES // 2, sums[0][f], sums[2][f]))
        return mains, ends

    def split_bits(t, carry):
        padded = pl.ds(pl.multiple_of(8 * t + 8, 8), 8)
        own = pl.ds(pl.multiple_of(8 * t, 8), 8)
        y = lax.broadcasted_iota(jnp.int32, (8, LANES), 0) + 8 * t
        beyond_z = jnp.where(lane8 == 0, bits_of(dz=-1), 0) | jnp.where(lane8 == LANES - 1, bits_of(dz=1), 0)
        beyond_y = jnp.where(y == 0, bits_of(dy=-1), 0) | jnp.where(y == ROWS - 1, bits_of(dy=1), 0)
        columns = jnp.zeros((8, LANES), jnp.int32)
        for x in range(LAYERS):
            active = act[x, padded, :]
            inner[x, own, :] = jnp.bitwise_and(active, jnp.bitwise_not(beyond_z | beyond_y))
            columns = packed(columns, active, x, lane8)
        columns = jnp.where(jnp.bitwise_and(lane8, 1) == 0, jnp.right_shift(columns, 2), columns)
        x = jnp.bitwise_and(jnp.right_shift(lane8, 1), LAYERS - 1)
        width = 2 * LAYERS
        wide = jnp.where(lane8 < width, columns, 0)
        for f in range(1, FIELDS):
            wide = jnp.where(jnp.right_shift(lane8, 3) == f, turn(columns, width * f), wide)
        beyond_x = jnp.where(x == 0, bits_of(dx=-1), 0) | jnp.where(x == LAYERS - 1, bits_of(dx=1), 0)
        ends_act[t] = jnp.bitwise_and(wide, jnp.bitwise_not(beyond_x | beyond_y))
        return carry

    def scatter(stage, count):
        which = stage // 2
        for sx in SIGNS:
            xt = -1 if sx == -1 else LAYERS
            ix = side(sx)
            for sy in SIGNS:
                mains, ends = pushed(xt, 0 if sy == -1 else PADDED - 8, (sy,), count)
                row = 7 if sy == -1 else 0
                e = 2 * ix + side(sy)
                pack = zero8
                for f in range(count):
                    edges[stage, e, f : f + 1, :] = mains[f][row : row + 1, :]
                    pack = packed(pack, ends[f], f, lane8)
                cpack[stage, e] = pack[row : row + 1, :]
        if stage == 0:
            pl.semaphore_wait(barrier, len(TRAVEL))
        send(stage, lambda sx, sy, sz, chunk: sx != 0 and sy != 0)
        for sx in SIGNS:
            xt = -1 if sx == -1 else LAYERS
            ix = side(sx)
            pack = zero8
            for t in range(TILES):
                mains, ends = pushed(xt, 8 * t + 8, (-1, 0, 1), count)
                for f in range(count):
                    xface[which, ix, f, 8 * t : 8 * t + 8, :] = mains[f]
                    pack = packed(pack, ends[f], count * t + f, lane8)
            xzpack[stage, ix] = pack
        send(stage, lambda sx, sy, sz, chunk: sx != 0 and sy == 0 and sz != 0)
        for chunk in ORDER:
            send(stage, faces((chunk,)))

        for sy in SIGNS:
            row = 7 if sy == -1 else 0
            pack = zero8
            for xt in range(LAYERS):
                mains, ends = pushed(xt, 0 if sy == -1 else PADDED - 8, (sy,), count)
                for f in range(count):
                    p = 4 * f + xt
                    yrows[stage, side(sy), p : p + 1, :] = mains[f][row : row + 1, :]
                    pack = packed(pack, ends[f], p, lane8)
            yzpack[stage, side(sy)] = pack[row : row + 1, :]
        send(stage, lambda sx, sy, sz, chunk: sx == 0 and sy != 0)
        if stage == 0:
            lax.fori_loop(0, TILES, split_bits, 0)

        def rest(pair, carry):
            pack = zero8
            for half in range(2):
                t = 2 * pair + half
                own = pl.ds(pl.multiple_of(8 * t, 8), 8)
                for xt in range(LAYERS):
                    mains, ends = pushed(xt, 8 * t + 8, (-1, 0, 1), count)
                    for f in range(count):
                        acc[f, xt, own, :] = mains[f]
                        pack = packed(pack, ends[f], 4 * f + xt + 32 * half, lane8)
            zpack[stage, pair] = pack
            return carry

        lax.fori_loop(0, TILES // 2, rest, 0)
        send(stage, lambda sx, sy, sz, chunk: (sx, sy) == (0, 0))

    def combine(stage, count):
        odd = stage + 1
        which = stage // 2

        def finish(x, t, sums):
            own = pl.ds(8 * t, 8)
            if stage == 0:
                inverse = 1.0 / sums[FIELDS]
                inv_volume[x, own, :] = inverse
            else:
                inverse = inv_volume[x, own, :]
            for f in range(FIELDS):
                hats[which, 1, f, x + 1, 8 * t + 8 : 8 * t + 16, :] = sums[f] * inverse

        receive(stage, 0)
        for sy in SIGNS:
            iy = side(sy)
            row = 0 if sy == 1 else ROWS - 1
            yz = pairs(ryz[stage, iy, 1], ryz[stage, iy, 0], lane1)
            for x in range(LAYERS):
                for f in range(count):
                    p = 4 * f + x
                    value = ry[stage, iy, p : p + 1, :] + only_ends(placed(yz, p), lane1)
                    acc[f, x, row : row + 1, :] += value
        for t in range(TILES):
            if t % 2 == 0:
                z = pairs(rz[stage, 1, t // 2], rz[stage, 0, t // 2], lane8)
            for x in range(LAYERS):
                sums = []
                for f in range(count):
                    value = acc[f, x, 8 * t : 8 * t + 8, :] + only_ends(placed(z, 4 * f + x + 32 * (t % 2)), lane8)
                    sums.append(value)
                if x in (0, LAYERS - 1):
                    for f in range(count):
                        acc[f, x, 8 * t : 8 * t + 8, :] = sums[f]
                else:
                    finish(x, t, sums)
        receive(stage, 1)
        for sx in SIGNS:
            ix = side(sx)
            x = 0 if sx == 1 else LAYERS - 1
            xz = pairs(rxz[stage, ix, 1], rxz[stage, ix, 0], lane8)
            for t in range(TILES):
                for f in range(count):
                    acc[f, x, 8 * t : 8 * t + 8, :] += only_ends(placed(xz, count * t + f), lane8)
            for sy in SIGNS:
                e = 2 * ix + side(sy)
                row = 0 if sy == 1 else ROWS - 1
                corner = pairs(rc[stage, e, 1], rc[stage, e, 0], lane1)
                for f in range(count):
                    value = re[stage, e, f : f + 1, :] + only_ends(placed(corner, f), lane1)
                    acc[f, x, row : row + 1, :] += value
        for position, chunk in enumerate(ORDER):
            receive(stage, 2 + chunk)
            for t in range(chunk * CHUNK // 8, (chunk + 1) * CHUNK // 8):
                for sx in SIGNS:
                    x = 0 if sx == 1 else LAYERS - 1
                    sums = []
                    for f in range(count):
                        own = slice(8 * t, 8 * t + 8)
                        sums.append(acc[f, x, own, :] + rx[which, side(sx), f, own, :])
                    finish(x, t, sums)
            if position == 1:
                for sx in SIGNS:
                    x = 0 if sx == -1 else LAYERS - 1
                    for sy in SIGNS:
                        row = 8 if sy == -1 else 7 + ROWS
                        e = 2 * side(sx) + side(sy)
                        pack = jnp.zeros((1, LANES), jnp.float32)
                        for f in range(FIELDS):
                            value = hats[which, 1, f, x + 1, row : row + 1, :]
                            edges[odd, e, f : f + 1, :] = value
                            pack = packed(pack, value, f, lane1)
                        cpack[odd, e] = pack
                send(odd, lambda sx, sy, sz, chunk: sx != 0 and sy != 0)
                for sy in SIGNS:
                    row = 8 if sy == -1 else 7 + ROWS
                    pack = jnp.zeros((1, LANES), jnp.float32)
                    for x in range(LAYERS):
                        for f in range(FIELDS):
                            p = 4 * f + x
                            value = hats[which, 1, f, x + 1, row : row + 1, :]
                            yrows[odd, side(sy), p : p + 1, :] = value
                            pack = packed(pack, value, p, lane1)
                    yzpack[odd, side(sy)] = pack
                send(odd, lambda sx, sy, sz, chunk: sx == 0 and sy != 0)
            if position == CHUNKS - 1:
                for sx in SIGNS:
                    x = 0 if sx == -1 else LAYERS - 1
                    pack = zero8
                    for t in range(TILES):
                        for f in range(FIELDS):
                            value = hats[which, 1, f, x + 1, 8 * t + 8 : 8 * t + 16, :]
                            pack = packed(pack, value, FIELDS * t + f, lane8)
                    xzpack[odd, side(sx)] = pack
                send(odd, lambda sx, sy, sz, chunk: sx != 0 and sy == 0 and sz != 0)
            send(odd, faces((chunk,)))
        for pair in range(TILES // 2):
            pack = zero8
            for t in (2 * pair, 2 * pair + 1):
                for x in range(LAYERS):
                    for f in range(FIELDS):
                        value = hats[which, 1, f, x + 1, 8 * t + 8 : 8 * t + 16, :]
                        pack = packed(pack, value, 4 * f + x + 32 * (t % 2), lane8)
            zpack[odd, pair] = pack
        send(odd, lambda sx, sy, sz, chunk: (sx, sy) == (0, 0))
        drain(stage)

    def gather(stage, last):
        which = stage // 2

        def shifted(f, xi, rows, value, ends, lane):
            hats[which, 2, f, xi, rows, :] = jnp.where(lane == LANES - 1, ends, turn(value, -1))
            hats[which, 0, f, xi, rows, :] = jnp.where(lane == 0, ends, turn(value, 1))

        def pulled(sums, x, t, dxs, active):
            for dx in dxs:
                if sums is None:
                    sums = [hats[which, 1, f, x + 1, pl.ds(8 * t + 8, 8), :] for f in range(FIELDS)]
                for dy in (-1, 0, 1):
                    for dz in (-1, 0, 1):
                        bit = offset_bit(dx, dy, dz)
                        if bit == 13:
                            continue
                        chosen = jnp.bitwise_and(active, 1 << bit) != 0
                        rows = pl.ds(8 * t + 8 + dy, 8)
                        for f in range(FIELDS):
                            value = hats[which, dz + 1, f, x + 1 + dx, rows, :]
                            sums[f] = sums[f] + jnp.where(chosen, value, 0.0)
            return sums

        def finish(x, t, sums):
            own = pl.ds(8 * t, 8)
            scale = inv_count[x, own, :]
            if not last:
                scale = scale * kap[x, own, :]
            for f in range(FIELDS):
                if last:
                    result[f, x, own, :] = sums[f] * scale
                else:
                    w[f, x, pl.ds(8 * t + 8, 8), :] = sums[f] * scale

        def rotations(t, carry):
            padded = pl.ds(pl.multiple_of(8 * t + 8, 8), 8)
            for x in range(LAYERS):
                for f in range(FIELDS):
                    value = hats[which, 1, f, x + 1, padded, :]
                    hats[which, 2, f, x + 1, padded, :] = turn(value, -1)
                    hats[which, 0, f, x + 1, padded, :] = turn(value, 1)
            return carry

        lax.fori_loop(0, TILES, rotations, 0)
        def interior(t, carry):
            own = pl.ds(pl.multiple_of(8 * t, 8), 8)
            for x in range(LAYERS):
                dxs = [dx for dx in (-1, 0, 1) if 0 <= x + dx < LAYERS]
                sums = pulled(None, x, t, dxs, inner[x, own, :])
                for f in range(FIELDS):
                    acc[f, x, own, :] = sums[f]
            return carry

        lax.fori_loop(0, TILES, interior, 0)
        receive(stage, 0)
        for sy in SIGNS:
            iy = side(sy)
            row = 7 if sy == 1 else 8 + ROWS
            yz = pairs(ryz[stage, iy, 1], ryz[stage, iy, 0], lane1)
            for x in range(LAYERS):
                for f in range(FIELDS):
                    p = 4 * f + x
                    value = ry[stage, iy, p : p + 1, :]
                    hats[which, 1, f, x + 1, row : row + 1, :] = value
                    shifted(f, x + 1, slice(row, row + 1), value, placed(yz, p), lane1)
        sublane = lax.broadcasted_iota(jnp.int32, (8, LANES), 0)
        for t, row, dy in ((0, 0, -1), (TILES - 1, 7, 1)):
            own = slice(8 * t, 8 * t + 8)
            for x in range(LAYERS):
                active = jnp.where(sublane == row, act[x, 8 * t + 8 : 8 * t + 16, :], 0)
                sums = [acc[f, x, own, :] for f in range(FIELDS)]
                for dx in (-1, 0, 1):
                    if not 0 <= x + dx < LAYERS:
                        continue
                    for dz in (-1, 0, 1):
                        chosen = jnp.bitwise_and(active, 1 << offset_bit(dx, dy, dz)) != 0
                        for f in range(FIELDS):
                            value = hats[which, dz + 1, f, x + 1 + dx, 8 * t + 8 + dy : 8 * t + 16 + dy, :]
                            sums[f] = sums[f] + jnp.where(chosen, value, 0.0)
                for f in range(FIELDS):
                    acc[f, x, own, :] = sums[f]
        for t in range(TILES):
            if t % 2 == 0:
                z = pairs(rz[stage, 1, t // 2], rz[stage, 0, t // 2], lane8)
            beyond[8 * t + 8 : 8 * t + 16, :] = turn(z, -64 * (t % 2))
        for t in range(TILES):
            active = ends_act[t]
            total = zero8
            for dy in (-1, 0, 1):
                values = beyond[8 * t + 8 + dy : 8 * t + 16 + dy, :]
                for dx in (-1, 0, 1):
                    chosen = jnp.bitwise_and(active, 1 << offset_bit(dx, dy, -1)) != 0
                    total = total + jnp.where(chosen, turn(values, -2 * dx), 0.0)
            for x in range(LAYERS):
                sums = []
                for f in range(FIELDS):
                    ends = only_ends(placed(total, 4 * f + x), lane8)
                    sums.append(acc[f, x, 8 * t : 8 * t + 8, :] + ends)
                if x in (0, LAYERS - 1):
                    for f in range(FIELDS):
                        acc[f, x, 8 * t : 8 * t + 8, :] = sums[f]
                else:
                    finish(x, t, sums)
        drain(stage)
        for group in range(1, 2 + CHUNKS):
            receive(stage, group)
        for sx in SIGNS:
            ix = side(sx)
            xi = 0 if sx == 1 else LAYERS + 1
            for sy in SIGNS:
                e = 2 * ix + side(sy)
                row = 7 if sy == 1 else 8 + ROWS
                corner = pairs(rc[stage, e, 1], rc[stage, e, 0], lane1)
                for f in range(FIELDS):
                    value = re[stage, e, f : f + 1, :]
                    hats[which, 1, f, xi, row : row + 1, :] = value
                    shifted(f, xi, slice(row, row + 1), value, placed(corner, f), lane1)
            xz = pairs(rxz[stage, ix, 1], rxz[stage, ix, 0], lane8)
            for t in range(TILES):
                rows = slice(8 * t + 8, 8 * t + 16)
                for f in range(FIELDS):
                    shifted(f, xi, rows, hats[which, 1, f, xi, rows, :], placed(xz, FIELDS * t + f), lane8)

        def boundary(t, carry):
            for x, dx in ((0, -1), (LAYERS - 1, 1)):
                sums = [acc[f, x, pl.ds(pl.multiple_of(8 * t, 8), 8), :] for f in range(FIELDS)]
                active = act[x, pl.ds(pl.multiple_of(8 * t + 8, 8), 8), :]
                finish(x, t, pulled(sums, x, t, (dx,), active))
            return carry

        lax.fori_loop(0, TILES, boundary, 0, unroll=4)

    scatter(0, FIELDS + 1)
    combine(0, FIELDS + 1)
    gather(1, False)
    scatter(2, FIELDS)
    combine(2, FIELDS)
    gather(3, True)


def body(fields, volume_code, cut_flag, member_bits):
    f32, i32 = jnp.float32, jnp.int32
    vmem = pltpu.VMEM
    block = (LAYERS, ROWS, LANES)
    padded = (LAYERS, PADDED, LANES)
    scratch = [
        vmem((FIELDS,) + block, f32),
        vmem(block, i32),
        vmem(block, i32),
        vmem(block, i32),
        vmem(padded, i32),
        vmem(block, f32),
        vmem(block, f32),
        vmem(block, f32),
        vmem((FIELDS + 1,) + padded, f32),
        vmem((FIELDS + 1,) + block, f32),
        vmem((2, 3, FIELDS, LAYERS + 2, PADDED, LANES), f32),
        vmem((2, 2, FIELDS + 1, ROWS, LANES), f32),
        vmem((4, 2, ROW_COUNT, LANES), f32),
        vmem((4, 4, 8, LANES), f32),
        vmem((4, TILES // 2, 8, LANES), f32),
        vmem((4, 2, 8, LANES), f32),
        vmem((4, 2, 1, LANES), f32),
        vmem((4, 4, 1, LANES), f32),
        vmem((2, 2, FIELDS + 1, ROWS, LANES), f32),
        vmem((4, 2, ROW_COUNT, LANES), f32),
        vmem((4, 4, 8, LANES), f32),
        vmem((4, 2, TILES // 2, 8, LANES), f32),
        vmem((4, 2, 2, 8, LANES), f32),
        vmem((4, 2, 2, 1, LANES), f32),
        vmem((4, 4, 2, 1, LANES), f32),
        pltpu.SemaphoreType.DMA((4,)),
        pltpu.SemaphoreType.DMA((4,)),
        pltpu.SemaphoreType.DMA((4, 2 + CHUNKS)),
        vmem((1024, 1, LANES), f32),
        vmem(block, i32),
        vmem((TILES, 8, LANES), i32),
        vmem((PADDED, LANES), f32),
    ]
    in_hbm = pl.BlockSpec(memory_space=pltpu.MemorySpace.HBM)
    in_vmem = pl.BlockSpec(memory_space=pltpu.MemorySpace.VMEM)
    operands = (fields, volume_code, cut_flag, member_bits)
    return pl.pallas_call(
        kernel,
        out_shape=jax.ShapeDtypeStruct((FIELDS,) + block, f32),
        in_specs=[in_hbm] * 4,
        out_specs=in_vmem,
        scratch_shapes=scratch,
        compiler_params=pltpu.CompilerParams(
            collective_id=0, has_side_effects=True, vmem_limit_bytes=52000000
        ),
    )(*[pltpu.with_memory_space_constraint(a, pltpu.MemorySpace.HBM) for a in operands])


def solution(mesh):
    in_specs = (
        P(None, "gx", "gy", "gz"),
        P("gx", "gy", "gz"),
        P("gx", "gy", "gz"),
        P("gx", "gy", "gz"),
    )
    out_specs = P(None, "gx", "gy", "gz")
    return jax.shard_map(body, mesh=mesh, in_specs=in_specs, out_specs=out_specs, check_vma=False)
```

```python
import jax
import jax.numpy as jnp
from jax import lax
from jax.experimental import pallas as pl
from jax.experimental.pallas import tpu as pltpu
from jax.sharding import PartitionSpec as P

MESH = pl.DeviceIdType.MESH
FIELDS = 4
LAYERS = 4
ROWS = 64
TILES = ROWS // 8
PADDED = ROWS + 16
LANES = 128
CHUNK = 8
CHUNKS = ROWS // CHUNK
ORDER = (1, 2, 0, CHUNKS - 1) + tuple(range(3, CHUNKS - 1))
ROW_COUNT = 24
SIGNS = (-1, 1)

TRAVEL = []
for kind in ((1, 0, 0), (1, 1, 0), (1, 0, 1), (1, 1, 1), (0, 0, 1), (0, 1, 0), (0, 1, 1)):
    for sx in SIGNS if kind[0] else (0,):
        for sy in SIGNS if kind[1] else (0,):
            for sz in SIGNS if kind[2] else (0,):
                TRAVEL.append((sx, sy, sz))
MESSAGES = []
for travel in TRAVEL:
    for chunk in range(CHUNKS if travel[1:] == (0, 0) else 1):
        MESSAGES.append(travel + (chunk,))


def side(sign):
    return (sign + 1) // 2


def offset_bit(dx, dy, dz):
    return 9 * (dx + 1) + 3 * (dy + 1) + (dz + 1)


def neighbour(travel):
    result = {}
    for axis, sign in zip(("gx", "gy", "gz"), travel):
        if sign:
            count = lax.axis_size(axis)
            result[axis] = lax.rem(lax.axis_index(axis) + sign + count, count)
    return result


def bits_of(dx=None, dy=None, dz=None):
    result = 0
    for x in (-1, 0, 1):
        for y in (-1, 0, 1):
            for z in (-1, 0, 1):
                if dx in (None, x) and dy in (None, y) and dz in (None, z):
                    result |= 1 << offset_bit(x, y, z)
    return result


def turn(value, shift):
    if isinstance(shift, int):
        shift = shift % LANES
        if shift == 0:
            return value
    return pltpu.roll(value, shift, 1)


def kernel(fields, volume_code, cut_flag, member_bits, result, raw, code, cut, bits, act, kap, inv_count,
           inv_volume, w, acc, hats, xface, yrows, edges, zpack, xzpack, yzpack, cpack,
           rx, ry, re, rz, rxz, ryz, rc, in_sem, send_sem, recv_sem, lengths, inner, ends_act, beyond):
    lane8 = lax.broadcasted_iota(jnp.int32, (8, LANES), 1)
    lane1 = lax.broadcasted_iota(jnp.int32, (1, LANES), 1)
    zero8 = jnp.zeros((8, LANES), jnp.float32)

    loads = []
    for index, (source, target) in enumerate(
        ((volume_code, code), (cut_flag, cut), (member_bits, bits), (fields, raw))
    ):
        copy = pltpu.make_async_copy(source, target, in_sem.at[index])
        copy.start()
        loads.append(copy)
    barrier = pltpu.get_barrier_semaphore()
    for travel in TRAVEL:
        pl.semaphore_signal(barrier, inc=1, device_id=neighbour(travel), device_id_type=MESH)

    for x in range(LAYERS):
        for rows in (0, PADDED - 8):
            act[x, rows : rows + 8, :] = jnp.zeros((8, LANES), jnp.int32)
            beyond[rows : rows + 8, :] = zero8
            for f in range(FIELDS + 1):
                w[f, x, rows : rows + 8, :] = zero8
    for copy in loads:
        copy.wait()

    def prepare(t, carry):
        own = pl.ds(pl.multiple_of(8 * t, 8), 8)
        padded = pl.ds(pl.multiple_of(8 * t + 8, 8), 8)
        for x in range(LAYERS):
            kappa = code[x, own, :].astype(jnp.float32) * (1.0 / 1048576.0)
            active = bits[x, own, :] * cut[x, own, :]
            act[x, padded, :] = active
            kap[x, own, :] = kappa
            others = lax.population_count(jnp.bitwise_and(active, ((1 << 27) - 1) ^ (1 << 13)))
            inv_count[x, own, :] = 1.0 / (others + 1).astype(jnp.float32)
            w[FIELDS, x, padded, :] = kappa
            for f in range(FIELDS):
                w[f, x, padded, :] = kappa * raw[f, x, own, :]
        return carry

    lax.fori_loop(0, TILES, prepare, 0)

    def message(stage, sx, sy, sz, chunk):
        count = FIELDS + 1 if stage == 0 else FIELDS
        which = stage // 2
        ix, iy, iz = side(sx), side(sy), side(sz)
        e = 2 * ix + iy
        if sx and not sy and not sz:
            start = chunk * CHUNK
            if stage % 2 == 0:
                source = xface.at[which, ix, 0:count, start : start + CHUNK, :]
                target = rx.at[which, ix, 0:count, start : start + CHUNK, :]
            else:
                mid = hats.at[which, 1]
                source = mid.at[:, 4 if sx == 1 else 1, 8 + start : 8 + start + CHUNK, :]
                target = mid.at[:, 0 if sx == 1 else 5, 8 + start : 8 + start + CHUNK, :]
        elif sy and not sx and not sz:
            source, target = yrows.at[stage, iy], ry.at[stage, iy]
        elif sz and not sx and not sy:
            source, target = zpack.at[stage], rz.at[stage, iz]
        elif sx and sy and not sz:
            source, target = edges.at[stage, e], re.at[stage, e]
        elif sx and sz and not sy:
            source, target = xzpack.at[stage, ix], rxz.at[stage, ix, iz]
        elif sy and sz and not sx:
            source, target = yzpack.at[stage, iy], ryz.at[stage, iy, iz]
        else:
            source, target = cpack.at[stage, e], rc.at[stage, e, iz]
        group = 0 if sx == 0 else 1 if sy else 2 if sz else 3 + chunk
        return pltpu.make_async_remote_copy(
            src_ref=source,
            dst_ref=target,
            send_sem=send_sem.at[stage],
            recv_sem=recv_sem.at[stage, group],
            device_id=neighbour((sx, sy, sz)),
            device_id_type=MESH,
        )

    def send(stage, chosen):
        for which in MESSAGES:
            if chosen(*which):
                message(stage, *which).start()

    def rows_of(stage, which):
        sx, sy, sz, chunk = which
        if (sy, sz) == (0, 0):
            return CHUNK * (FIELDS + 1 if stage == 0 else FIELDS)
        if (sx, sz) == (0, 0):
            return ROW_COUNT
        if (sx, sy) == (0, 0):
            return ROWS // 2
        return 8 if sx and not (sy and sz) else 1

    def await_rows(semaphore, rows):
        part = lengths.at[0:rows]
        pltpu.make_async_copy(part, part, semaphore).wait()

    def receive(stage, group):
        chosen = [beside, corner, column, None][min(group, 3)] or faces((group - 3,))
        rows = sum(rows_of(stage, which) for which in MESSAGES if chosen(*which))
        await_rows(recv_sem.at[stage, group], rows)

    def drain(stage):
        await_rows(send_sem.at[stage], sum(rows_of(stage, which) for which in MESSAGES))

    def beside(sx, sy, sz, chunk):
        return sx == 0

    def corner(sx, sy, sz, chunk):
        return sx != 0 and sy != 0

    def column(sx, sy, sz, chunk):
        return sx != 0 and sy == 0 and sz != 0

    def faces(wanted):
        return lambda sx, sy, sz, chunk: sx != 0 and sy == 0 and sz == 0 and chunk in wanted

    def packed(base, value, p, lane):
        return jnp.where(jnp.right_shift(lane, 1) == p, turn(value, 1 + 2 * p), base)

    def pairs(from_below, from_above, lane):
        return jnp.where(jnp.bitwise_and(lane, 1) == 1, turn(from_below, 1), turn(from_above, -1))

    def placed(pack, p):
        return turn(pack, LANES - 1 - 2 * p)

    def only_ends(value, lane):
        return jnp.where((lane == 0) | (lane == LANES - 1), value, 0.0)

    def pushed(xt, row, dys, count):
        sums = [[None] * count for _ in range(3)]
        for dx in (-1, 0, 1):
            xs = xt - dx
            if xs < 0 or xs >= LAYERS:
                continue
            for dy in dys:
                rows = pl.ds(row - dy, 8)
                active = act[xs, rows, :]
                values = [w[f, xs, rows, :] for f in range(count)]
                for dz in (-1, 0, 1):
                    bit = offset_bit(dx, dy, dz)
                    if bit != 13:
                        chosen = jnp.bitwise_and(active, 1 << bit) != 0
                    for f in range(count):
                        term = values[f] if bit == 13 else jnp.where(chosen, values[f], 0.0)
                        old = sums[dz + 1][f]
                        sums[dz + 1][f] = term if old is None else old + term
        mains, ends = [], []
        for f in range(count):
            up = turn(sums[2][f], 1)
            down = turn(sums[0][f], -1)
            mains.append(
                sums[1][f] + jnp.where(lane8 == 0, 0.0, up) + jnp.where(lane8 == LANES - 1, 0.0, down)
            )
            ends.append(jnp.where(lane8 < LANES // 2, sums[0][f], sums[2][f]))
        return mains, ends

    def split_bits(t, carry):
        padded = pl.ds(pl.multiple_of(8 * t + 8, 8), 8)
        own = pl.ds(pl.multiple_of(8 * t, 8), 8)
        y = lax.broadcasted_iota(jnp.int32, (8, LANES), 0) + 8 * t
        beyond_z = jnp.where(lane8 == 0, bits_of(dz=-1), 0) | jnp.where(lane8 == LANES - 1, bits_of(dz=1), 0)
        beyond_y = jnp.where(y == 0, bits_of(dy=-1), 0) | jnp.where(y == ROWS - 1, bits_of(dy=1), 0)
        columns = jnp.zeros((8, LANES), jnp.int32)
        for x in range(LAYERS):
            active = act[x, padded, :]
            inner[x, own, :] = jnp.bitwise_and(active, jnp.bitwise_not(beyond_z | beyond_y))
            columns = packed(columns, active, x, lane8)
        columns = jnp.where(jnp.bitwise_and(lane8, 1) == 0, jnp.right_shift(columns, 2), columns)
        x = jnp.bitwise_and(jnp.right_shift(lane8, 1), LAYERS - 1)
        width = 2 * LAYERS
        wide = jnp.where(lane8 < width, columns, 0)
        for f in range(1, FIELDS):
            wide = jnp.where(jnp.right_shift(lane8, 3) == f, turn(columns, width * f), wide)
        beyond_x = jnp.where(x == 0, bits_of(dx=-1), 0) | jnp.where(x == LAYERS - 1, bits_of(dx=1), 0)
        ends_act[t] = jnp.bitwise_and(wide, jnp.bitwise_not(beyond_x | beyond_y))
        return carry

    def scatter_edges(stage, count):
        for sx in SIGNS:
            xt = -1 if sx == -1 else LAYERS
            ix = side(sx)
            for sy in SIGNS:
                mains, ends = pushed(xt, 0 if sy == -1 else PADDED - 8, (sy,), count)
                row = 7 if sy == -1 else 0
                e = 2 * ix + side(sy)
                pack = zero8
                for f in range(count):
                    edges[stage, e, f : f + 1, :] = mains[f][row : row + 1, :]
                    pack = packed(pack, ends[f], f, lane8)
                cpack[stage, e] = pack[row : row + 1, :]
        if stage == 0:
            pl.semaphore_wait(barrier, len(TRAVEL))
        send(stage, lambda sx, sy, sz, chunk: sx != 0 and sy != 0)

    def scatter(stage, count):
        which = stage // 2
        for sx in SIGNS:
            xt = -1 if sx == -1 else LAYERS
            ix = side(sx)
            pack = zero8
            for t in range(TILES):
                mains, ends = pushed(xt, 8 * t + 8, (-1, 0, 1), count)
                for f in range(count):
                    xface[which, ix, f, 8 * t : 8 * t + 8, :] = mains[f]
                    pack = packed(pack, ends[f], count * t + f, lane8)
            xzpack[stage, ix] = pack
        send(stage, lambda sx, sy, sz, chunk: sx != 0 and sy == 0 and sz != 0)
        for chunk in ORDER:
            send(stage, faces((chunk,)))

        for sy in SIGNS:
            row = 7 if sy == -1 else 0
            pack = zero8
            for xt in range(LAYERS):
                mains, ends = pushed(xt, 0 if sy == -1 else PADDED - 8, (sy,), count)
                for f in range(count):
                    p = 4 * f + xt
                    yrows[stage, side(sy), p : p + 1, :] = mains[f][row : row + 1, :]
                    pack = packed(pack, ends[f], p, lane8)
            yzpack[stage, side(sy)] = pack[row : row + 1, :]
        send(stage, lambda sx, sy, sz, chunk: sx == 0 and sy != 0)
        def rest(pair, carry):
            pack = zero8
            for half in range(2):
                t = 2 * pair + half
                own = pl.ds(pl.multiple_of(8 * t, 8), 8)
                for xt in range(LAYERS):
                    mains, ends = pushed(xt, 8 * t + 8, (-1, 0, 1), count)
                    for f in range(count):
                        acc[f, xt, own, :] = mains[f]
                        pack = packed(pack, ends[f], 4 * f + xt + 32 * half, lane8)
            zpack[stage, pair] = pack
            return carry

        lax.fori_loop(0, TILES // 2, rest, 0)
        send(stage, lambda sx, sy, sz, chunk: (sx, sy) == (0, 0))
        if stage == 0:
            lax.fori_loop(0, TILES, split_bits, 0)

    def combine(stage, count):
        odd = stage + 1
        which = stage // 2

        def finish(x, t, sums):
            own = pl.ds(8 * t, 8)
            if stage == 0:
                inverse = 1.0 / sums[FIELDS]
                inv_volume[x, own, :] = inverse
            else:
                inverse = inv_volume[x, own, :]
            for f in range(FIELDS):
                hats[which, 1, f, x + 1, 8 * t + 8 : 8 * t + 16, :] = sums[f] * inverse

        receive(stage, 0)
        for sy in SIGNS:
            iy = side(sy)
            row = 0 if sy == 1 else ROWS - 1
            yz = pairs(ryz[stage, iy, 1], ryz[stage, iy, 0], lane1)
            for x in range(LAYERS):
                for f in range(count):
                    p = 4 * f + x
                    value = ry[stage, iy, p : p + 1, :] + only_ends(placed(yz, p), lane1)
                    acc[f, x, row : row + 1, :] += value
        def z_ends(layers):
            for t in range(TILES):
                if t % 2 == 0:
                    z = pairs(rz[stage, 1, t // 2], rz[stage, 0, t // 2], lane8)
                for x in layers:
                    sums = []
                    for f in range(count):
                        ends = only_ends(placed(z, 4 * f + x + 32 * (t % 2)), lane8)
                        sums.append(acc[f, x, 8 * t : 8 * t + 8, :] + ends)
                    if x in (0, LAYERS - 1):
                        for f in range(count):
                            acc[f, x, 8 * t : 8 * t + 8, :] = sums[f]
                    else:
                        finish(x, t, sums)

        z_ends((0, LAYERS - 1))
        receive(stage, 2)
        for sx in SIGNS:
            ix = side(sx)
            x = 0 if sx == 1 else LAYERS - 1
            xz = pairs(rxz[stage, ix, 1], rxz[stage, ix, 0], lane8)
            for t in range(TILES):
                for f in range(count):
                    acc[f, x, 8 * t : 8 * t + 8, :] += only_ends(placed(xz, count * t + f), lane8)

        def corner_rows():
            receive(stage, 1)
            for sx in SIGNS:
                ix = side(sx)
                x = 0 if sx == 1 else LAYERS - 1
                for sy in SIGNS:
                    e = 2 * ix + side(sy)
                    row = 0 if sy == 1 else ROWS - 1
                    corner = pairs(rc[stage, e, 1], rc[stage, e, 0], lane1)
                    for f in range(count):
                        value = re[stage, e, f : f + 1, :] + only_ends(placed(corner, f), lane1)
                        acc[f, x, row : row + 1, :] += value

        for position, chunk in enumerate(ORDER):
            if chunk == 0:
                corner_rows()
            receive(stage, 3 + chunk)
            for t in (chunk,):
                for sx in SIGNS:
                    x = 0 if sx == 1 else LAYERS - 1
                    sums = []
                    for f in range(count):
                        own = slice(8 * t, 8 * t + 8)
                        sums.append(acc[f, x, own, :] + rx[which, side(sx), f, own, :])
                    finish(x, t, sums)
            if position == 3:
                for sx in SIGNS:
                    x = 0 if sx == -1 else LAYERS - 1
                    for sy in SIGNS:
                        row = 8 if sy == -1 else 7 + ROWS
                        e = 2 * side(sx) + side(sy)
                        pack = jnp.zeros((1, LANES), jnp.float32)
                        for f in range(FIELDS):
                            value = hats[which, 1, f, x + 1, row : row + 1, :]
                            edges[odd, e, f : f + 1, :] = value
                            pack = packed(pack, value, f, lane1)
                        cpack[odd, e] = pack
                send(odd, lambda sx, sy, sz, chunk: sx != 0 and sy != 0)
                send(odd, faces((chunk,)))
                for sy in SIGNS:
                    row = 8 if sy == -1 else 7 + ROWS
                    pack = jnp.zeros((1, LANES), jnp.float32)
                    for x in range(LAYERS):
                        for f in range(FIELDS):
                            p = 4 * f + x
                            value = hats[which, 1, f, x + 1, row : row + 1, :]
                            yrows[odd, side(sy), p : p + 1, :] = value
                            pack = packed(pack, value, p, lane1)
                    yzpack[odd, side(sy)] = pack
                send(odd, lambda sx, sy, sz, chunk: sx == 0 and sy != 0)
            if position == CHUNKS - 1:
                for sx in SIGNS:
                    x = 0 if sx == -1 else LAYERS - 1
                    pack = zero8
                    for t in range(TILES):
                        for f in range(FIELDS):
                            value = hats[which, 1, f, x + 1, 8 * t + 8 : 8 * t + 16, :]
                            pack = packed(pack, value, FIELDS * t + f, lane8)
                    xzpack[odd, side(sx)] = pack
                send(odd, lambda sx, sy, sz, chunk: sx != 0 and sy == 0 and sz != 0)
            if position != 3:
                send(odd, faces((chunk,)))
            if position < 2:
                z_ends((position + 1,))
        for pair in range(TILES // 2):
            pack = zero8
            for t in (2 * pair, 2 * pair + 1):
                for x in range(LAYERS):
                    for f in range(FIELDS):
                        value = hats[which, 1, f, x + 1, 8 * t + 8 : 8 * t + 16, :]
                        pack = packed(pack, value, 4 * f + x + 32 * (t % 2), lane8)
            zpack[odd, pair] = pack
        send(odd, lambda sx, sy, sz, chunk: (sx, sy) == (0, 0))

    def gather(stage, last, between):
        which = stage // 2

        def shifted(f, xi, rows, value, ends, lane):
            hats[which, 2, f, xi, rows, :] = jnp.where(lane == LANES - 1, ends, turn(value, -1))
            hats[which, 0, f, xi, rows, :] = jnp.where(lane == 0, ends, turn(value, 1))

        def pulled(sums, x, t, dxs, active):
            for dx in dxs:
                if sums is None:
                    sums = [hats[which, 1, f, x + 1, pl.ds(8 * t + 8, 8), :] for f in range(FIELDS)]
                for dy in (-1, 0, 1):
                    for dz in (-1, 0, 1):
                        bit = offset_bit(dx, dy, dz)
                        if bit == 13:
                            continue
                        chosen = jnp.bitwise_and(active, 1 << bit) != 0
                        rows = pl.ds(8 * t + 8 + dy, 8)
                        for f in range(FIELDS):
                            value = hats[which, dz + 1, f, x + 1 + dx, rows, :]
                            sums[f] = sums[f] + jnp.where(chosen, value, 0.0)
            return sums

        def finish(x, t, sums):
            own = pl.ds(8 * t, 8)
            scale = inv_count[x, own, :]
            if not last:
                scale = scale * kap[x, own, :]
            for f in range(FIELDS):
                if last:
                    result[f, x, own, :] = sums[f] * scale
                else:
                    w[f, x, pl.ds(8 * t + 8, 8), :] = sums[f] * scale

        def rotations(t, carry):
            padded = pl.ds(pl.multiple_of(8 * t + 8, 8), 8)
            for x in range(LAYERS):
                for f in range(FIELDS):
                    value = hats[which, 1, f, x + 1, padded, :]
                    hats[which, 2, f, x + 1, padded, :] = turn(value, -1)
                    hats[which, 0, f, x + 1, padded, :] = turn(value, 1)
            return carry

        lax.fori_loop(0, TILES, rotations, 0)
        def interior(t, carry):
            own = pl.ds(pl.multiple_of(8 * t, 8), 8)
            for x in range(LAYERS):
                dxs = [dx for dx in (-1, 0, 1) if 0 <= x + dx < LAYERS]
                sums = pulled(None, x, t, dxs, inner[x, own, :])
                for f in range(FIELDS):
                    acc[f, x, own, :] = sums[f]
            return carry

        lax.fori_loop(0, TILES, interior, 0)
        receive(stage, 0)
        for sy in SIGNS:
            iy = side(sy)
            row = 7 if sy == 1 else 8 + ROWS
            yz = pairs(ryz[stage, iy, 1], ryz[stage, iy, 0], lane1)
            for x in range(LAYERS):
                for f in range(FIELDS):
                    p = 4 * f + x
                    value = ry[stage, iy, p : p + 1, :]
                    hats[which, 1, f, x + 1, row : row + 1, :] = value
                    shifted(f, x + 1, slice(row, row + 1), value, placed(yz, p), lane1)
        sublane = lax.broadcasted_iota(jnp.int32, (8, LANES), 0)
        for t, row, dy in ((0, 0, -1), (TILES - 1, 7, 1)):
            own = slice(8 * t, 8 * t + 8)
            for x in range(LAYERS):
                active = jnp.where(sublane == row, act[x, 8 * t + 8 : 8 * t + 16, :], 0)
                sums = [acc[f, x, own, :] for f in range(FIELDS)]
                for dx in (-1, 0, 1):
                    if not 0 <= x + dx < LAYERS:
                        continue
                    for dz in (-1, 0, 1):
                        chosen = jnp.bitwise_and(active, 1 << offset_bit(dx, dy, dz)) != 0
                        for f in range(FIELDS):
                            value = hats[which, dz + 1, f, x + 1 + dx, 8 * t + 8 + dy : 8 * t + 16 + dy, :]
                            sums[f] = sums[f] + jnp.where(chosen, value, 0.0)
                for f in range(FIELDS):
                    acc[f, x, own, :] = sums[f]
        for t in range(TILES):
            if t % 2 == 0:
                z = pairs(rz[stage, 1, t // 2], rz[stage, 0, t // 2], lane8)
            beyond[8 * t + 8 : 8 * t + 16, :] = turn(z, -64 * (t % 2))
        for t in range(TILES):
            active = ends_act[t]
            total = zero8
            for dy in (-1, 0, 1):
                values = beyond[8 * t + 8 + dy : 8 * t + 16 + dy, :]
                for dx in (-1, 0, 1):
                    chosen = jnp.bitwise_and(active, 1 << offset_bit(dx, dy, -1)) != 0
                    total = total + jnp.where(chosen, turn(values, -2 * dx), 0.0)
            for x in range(LAYERS):
                sums = []
                for f in range(FIELDS):
                    ends = only_ends(placed(total, 4 * f + x), lane8)
                    sums.append(acc[f, x, 8 * t : 8 * t + 8, :] + ends)
                if x in (0, LAYERS - 1):
                    for f in range(FIELDS):
                        acc[f, x, 8 * t : 8 * t + 8, :] = sums[f]
                else:
                    finish(x, t, sums)
        drain(stage - 1)
        for group in range(1, 3 + CHUNKS):
            receive(stage, group)
        for sx in SIGNS:
            ix = side(sx)
            xi = 0 if sx == 1 else LAYERS + 1
            for sy in SIGNS:
                e = 2 * ix + side(sy)
                row = 7 if sy == 1 else 8 + ROWS
                corner = pairs(rc[stage, e, 1], rc[stage, e, 0], lane1)
                for f in range(FIELDS):
                    value = re[stage, e, f : f + 1, :]
                    hats[which, 1, f, xi, row : row + 1, :] = value
                    shifted(f, xi, slice(row, row + 1), value, placed(corner, f), lane1)
            xz = pairs(rxz[stage, ix, 1], rxz[stage, ix, 0], lane8)
            for t in range(TILES):
                rows = slice(8 * t + 8, 8 * t + 16)
                for f in range(FIELDS):
                    shifted(f, xi, rows, hats[which, 1, f, xi, rows, :], placed(xz, FIELDS * t + f), lane8)

        def boundary(t, carry):
            for x, dx in ((0, -1), (LAYERS - 1, 1)):
                sums = [acc[f, x, pl.ds(8 * t, 8), :] for f in range(FIELDS)]
                active = act[x, pl.ds(8 * t + 8, 8), :]
                finish(x, t, pulled(sums, x, t, (dx,), active))
            return carry

        boundary(0, 0)
        boundary(TILES - 1, 0)
        between()
        lax.fori_loop(1, TILES - 1, boundary, 0, unroll=3)

    scatter_edges(0, FIELDS + 1)
    scatter(0, FIELDS + 1)
    combine(0, FIELDS + 1)
    gather(1, False, lambda: scatter_edges(2, FIELDS))
    scatter(2, FIELDS)
    combine(2, FIELDS)
    gather(3, True, lambda: None)
    drain(1)
    drain(3)


def body(fields, volume_code, cut_flag, member_bits):
    f32, i32 = jnp.float32, jnp.int32
    vmem = pltpu.VMEM
    block = (LAYERS, ROWS, LANES)
    padded = (LAYERS, PADDED, LANES)
    scratch = [
        vmem((FIELDS,) + block, f32),
        vmem(block, i32),
        vmem(block, i32),
        vmem(block, i32),
        vmem(padded, i32),
        vmem(block, f32),
        vmem(block, f32),
        vmem(block, f32),
        vmem((FIELDS + 1,) + padded, f32),
        vmem((FIELDS + 1,) + block, f32),
        vmem((2, 3, FIELDS, LAYERS + 2, PADDED, LANES), f32),
        vmem((2, 2, FIELDS + 1, ROWS, LANES), f32),
        vmem((4, 2, ROW_COUNT, LANES), f32),
        vmem((4, 4, 8, LANES), f32),
        vmem((4, TILES // 2, 8, LANES), f32),
        vmem((4, 2, 8, LANES), f32),
        vmem((4, 2, 1, LANES), f32),
        vmem((4, 4, 1, LANES), f32),
        vmem((2, 2, FIELDS + 1, ROWS, LANES), f32),
        vmem((4, 2, ROW_COUNT, LANES), f32),
        vmem((4, 4, 8, LANES), f32),
        vmem((4, 2, TILES // 2, 8, LANES), f32),
        vmem((4, 2, 2, 8, LANES), f32),
        vmem((4, 2, 2, 1, LANES), f32),
        vmem((4, 4, 2, 1, LANES), f32),
        pltpu.SemaphoreType.DMA((4,)),
        pltpu.SemaphoreType.DMA((4,)),
        pltpu.SemaphoreType.DMA((4, 3 + CHUNKS)),
        vmem((1024, 1, LANES), f32),
        vmem(block, i32),
        vmem((TILES, 8, LANES), i32),
        vmem((PADDED, LANES), f32),
    ]
    in_hbm = pl.BlockSpec(memory_space=pltpu.MemorySpace.HBM)
    in_vmem = pl.BlockSpec(memory_space=pltpu.MemorySpace.VMEM)
    operands = (fields, volume_code, cut_flag, member_bits)
    return pl.pallas_call(
        kernel,
        out_shape=jax.ShapeDtypeStruct((FIELDS,) + block, f32),
        in_specs=[in_hbm] * 4,
        out_specs=in_vmem,
        scratch_shapes=scratch,
        compiler_params=pltpu.CompilerParams(
            collective_id=0, has_side_effects=True, vmem_limit_bytes=52000000
        ),
    )(*[pltpu.with_memory_space_constraint(a, pltpu.MemorySpace.HBM) for a in operands])


def solution(mesh):
    in_specs = (
        P(None, "gx", "gy", "gz"),
        P("gx", "gy", "gz"),
        P("gx", "gy", "gz"),
        P("gx", "gy", "gz"),
    )
    out_specs = P(None, "gx", "gy", "gz")
    return jax.shard_map(body, mesh=mesh, in_specs=in_specs, out_specs=out_specs, check_vma=False)
```
